256 devices in a mesh: rows: 32 (over z, x), feat: 8 (over y, core).
Axes of the slice: x: 4, y: 4, z: 8, core: 2. Of those that a mesh axis runs over, the one named last changes fastest.
Arguments:
- tile_values: bfloat16 [8192, 512, 128], P('rows', 'feat'), may hold values from -6 to 6
- tile_blocks: int32 [8192, 512], P('rows', 'feat'), may hold values from 0 to 1023
- tile_counts: int32 [8192, 8], P('rows', 'feat'), may hold values from 1 to 64, as said below
- labels: int32 [8192], P('rows'), may hold values 0 or 1
- owner_rank: int32 [8192], P('rows'), may hold values from 0 to 31, as said below
- weights: float32 [8192, 128], P(('feat', 'rows')), may hold values from -0.09375 to 0.09375
Outputs:
- owned_margins: float32 [8192], P('rows')
- gradient: float32 [8192, 128], P(('feat', 'rows'))
- loss: float32 [], replicated
The draws below stay inside these ranges and needn't reach their ends.
Inputs may be any that keep to these rules, and one draw needn't show every extreme that they name: `owner_rank`: within each aligned block of 256 examples, every owner is named by exactly 8 examples. `tile_counts`: in every aligned block of 256 examples, each shard's column holds at least one example with exactly 64 used slots.
All inputs are finite; a program needn't handle non-finite values. No bound on the sum of `labels` on one device may be relied on, other than what follows from the above.
Results may differ from the reference program's by a relative error of at most 0.003.
Values may be sent and summed in bfloat16 or wider, within the bound.
No kernel may reach another device: no remote copies, remote signals or barrier semaphores. Data moves between devices by JAX's collectives and lax.ppermute only.
A program may use at most 64 MiB of HBM per device.

```python
import jax
import jax.numpy as jnp
from jax import lax

TILE = 128
EX_DEV = 256
TPAD = 64
EXAMPLES = 8192
SLOTS = 512
NBLK = 8192
BLK_SHARD = 1024
PER_PEER = 8
N_ROWS = 32
N_FEAT = 8


def draw_tile_counts(key, part):
    device_count = EXAMPLES // EX_DEV
    shard_count = SLOTS // TPAD
    key_shift = jax.random.fold_in(key, 11)
    key_value = jax.random.fold_in(key, 12)
    key_full = jax.random.fold_in(key, 13)
    device_of = jnp.arange(EXAMPLES, dtype=jnp.int32) // EX_DEV
    spread = max(device_count - 1, 1)
    ceiling = TPAD * (spread + 2 * device_of) // (3 * spread)
    ceiling = jnp.maximum(ceiling, 1)
    shifts = jax.random.randint(key_shift, (EXAMPLES, shard_count), 0, 4)
    divisor = jnp.left_shift(jnp.ones_like(shifts), shifts)
    upper = jnp.maximum(ceiling[:, None] // divisor, 1)
    raw_value = jax.random.randint(key_value, (EXAMPLES, shard_count), 0, 1048576)
    drawn = raw_value % upper + 1
    chosen = jax.random.randint(key_full, (device_count, shard_count), 0, EX_DEV)
    local_index = jnp.arange(EXAMPLES, dtype=jnp.int32) % EX_DEV
    marked = local_index[:, None] == jnp.repeat(chosen, EX_DEV, axis=0)
    return jnp.where(marked, TPAD, drawn).astype(jnp.int32)


def one_block_owner(block_key):
    return jax.random.permutation(block_key, EX_DEV)


def draw_owner_rank(key, part):
    device_count = EXAMPLES // EX_DEV
    block_keys = jax.random.split(jax.random.fold_in(key, 21), device_count)
    shuffled = jax.vmap(one_block_owner)(block_keys)
    return (shuffled // PER_PEER).reshape(EXAMPLES).astype(jnp.int32)


def set_ends(values, key, smallest, high):
    extent = values.shape
    place = [jax.random.randint(jax.random.fold_in(key, axis), (), 0, extent[axis]) for axis in range(len(extent))]
    values = values.at[tuple(place)].set(smallest)
    longest = extent.index(max(extent))
    place[longest] = (place[longest] + 1) % extent[longest]
    return values.at[tuple(place)].set(high)


def levels(rng, dims, pieces, smallest, largest):
    def one(dim, blocks):
        draws = jax.random.uniform(jax.random.fold_in(jax.random.fold_in(rng, 6), dim), (blocks,), jnp.float32, smallest / len(pieces), largest / len(pieces))
        return jnp.repeat(jnp.exp(draws), dims[dim] // blocks).reshape((-1,) + (1,) * (len(dims) - dim - 1))

    factor_of = one(*pieces[0])
    for cut in pieces[1:]:
        factor_of = factor_of * one(*cut)
    return factor_of


def bell_draw(stream_key, dims, width, bound, cuts=(), held_as=jnp.bfloat16):
    loudness = levels(stream_key, dims, cuts, -0.22, 0.18) if cuts else 1.0
    array = jax.random.normal(stream_key, dims, jnp.float32) * width * loudness
    return jnp.minimum(jnp.maximum(array, -bound), bound).astype(held_as)


def setup_inputs(seed: int = 0) -> dict:
    splits = jax.random.split(jax.random.key(seed), 7)
    return {
        "tile_values": bell_draw(splits[0], (EXAMPLES, SLOTS, TILE), 1.0, 6.0, ((0, 32), (1, 8))),
        "tile_blocks": set_ends(jax.random.randint(splits[1], (EXAMPLES, SLOTS), 0, BLK_SHARD), jax.random.fold_in(splits[1], 1), 0, BLK_SHARD - 1).astype(jnp.int32),
        "tile_counts": draw_tile_counts(jax.random.fold_in(splits[6], 71), 0),
        "labels": set_ends((jax.random.randint(splits[3], (EXAMPLES,), 0, 2) < 1).astype(jnp.int32), jax.random.fold_in(splits[3], 1), 0, 1),
        "owner_rank": draw_owner_rank(jax.random.fold_in(splits[6], 71), 0),
        "weights": bell_draw(splits[5], (NBLK, TILE), (TPAD * TPAD) ** -0.5, 0.09375, ((0, 256),), jnp.float32),
    }


def reference(tile_values, tile_blocks, tile_counts, labels, owner_rank, weights):
    w_half = weights.astype(jnp.bfloat16)
    slot_index = jnp.arange(TPAD, dtype=jnp.int32)

    def shard_pieces(shard_index):
        values = lax.dynamic_slice_in_dim(tile_values, shard_index * TPAD, TPAD, 1)
        block_ids = lax.dynamic_slice_in_dim(tile_blocks, shard_index * TPAD, TPAD, 1)
        used = lax.dynamic_slice_in_dim(tile_counts, shard_index, 1, 1)
        live_slot = slot_index[None, :] < used
        return values, block_ids, live_slot

    def shard_margin(shard_index):
        values, block_ids, live_slot = shard_pieces(shard_index)
        weight_table = lax.dynamic_slice_in_dim(w_half, shard_index * BLK_SHARD, BLK_SHARD, 0)
        picked = weight_table[block_ids]
        products = jnp.sum(values.astype(jnp.float32) * picked.astype(jnp.float32), axis=2)
        return jnp.sum(jnp.where(live_slot, products, jnp.float32(0.0)), axis=1)

    shard_index_all = jnp.arange(N_FEAT, dtype=jnp.int32)
    partials = lax.map(shard_margin, shard_index_all)
    margin = jnp.sum(partials, axis=0)
    label_float = labels.astype(jnp.float32)
    residual = jax.nn.sigmoid(margin) - label_float
    loss = jnp.sum(jax.nn.softplus(margin) - label_float * margin) / EXAMPLES
    resid_half = residual.astype(jnp.bfloat16)

    def shard_gradient(shard_index):
        values, block_ids, live_slot = shard_pieces(shard_index)
        coefficient = jnp.where(live_slot, resid_half[:, None], jnp.zeros((), jnp.bfloat16))
        weighted = values.astype(jnp.float32) * coefficient.astype(jnp.float32)[:, :, None]
        return jax.ops.segment_sum(weighted.reshape(-1, TILE), block_ids.reshape(-1), num_segments=BLK_SHARD)

    gradient = lax.map(shard_gradient, shard_index_all).reshape(NBLK, TILE)
    owners = owner_rank.reshape(N_ROWS, EX_DEV)
    send_order = jnp.argsort(owners, axis=1, stable=True).astype(jnp.int32)
    source = send_order + (jnp.arange(N_ROWS, dtype=jnp.int32) * EX_DEV)[:, None]
    source = jnp.transpose(source.reshape(N_ROWS, N_ROWS, PER_PEER), (1, 0, 2)).reshape(EXAMPLES)
    owned_margins = margin[source]
    return owned_margins, gradient, loss
```

```python
import jax
import jax.numpy as jnp
from jax import lax
from jax.experimental import pallas as pl
from jax.experimental.pallas import tpu as pltpu
from jax.sharding import PartitionSpec as P

F32 = jnp.float32
BF16 = jnp.bfloat16
I32 = jnp.int32

E = 256
SLOT = 64
C = 128
B = 1024
R = 32
F = 8
OWN = 8
GR = 8
NG = E * SLOT // GR
CH = 256
GCH = CH // GR
NCH = NG // GCH
XR = 8
LOADS = 4

VMEM = pl.BlockSpec(memory_space=pltpu.VMEM)
SMEM = pl.BlockSpec(memory_space=pltpu.SMEM)
ANY = pl.BlockSpec(memory_space=pl.ANY)


def nt(a, b):
    return lax.dot_general(a, b, (((1,), (1,)), ((), ())), preferred_element_type=F32)


def nn(a, b):
    return lax.dot_general(a, b, (((1,), (0,)), ((), ())), preferred_element_type=F32)


def split3(x):
    hi = x.astype(BF16).astype(F32)
    mid = (x - hi).astype(BF16).astype(F32)
    lo = (x - hi - mid).astype(BF16).astype(F32)
    return hi, mid, lo


def iota(shape, dim):
    return lax.broadcasted_iota(I32, shape, dim)


def spread_weights(w_ref, out_ref):
    out_ref[...] = jnp.broadcast_to(w_ref[...].astype(BF16)[None], out_ref.shape)


def pack_tiles(
    counts_s, counts_ref, blocks_ref, owner_ref, values_hbm, packed_hbm, ids_ref, ex_ref, rank_ref,
    total_ref, values, packed_ref, sems, out_sem
):
    part = NG // LOADS

    def load(i):
        return pltpu.make_async_copy(
            values_hbm.at[pl.ds(i * part, part)], values.at[pl.ds(i * part, part)], sems.at[i]
        )

    for i in range(LOADS):
        load(i).start()

    counts = counts_ref[...]
    granules = lax.shift_right_logical(counts + (GR - 1), 3).astype(F32)
    spread = jnp.broadcast_to(granules, (E, E)).astype(BF16)
    up = iota((E, E), 0)
    across = iota((E, E), 1)
    first = nt((across < up).astype(F32).astype(BF16), spread)
    last = nt((across <= up).astype(F32).astype(BF16), spread)
    before = (up < across).astype(F32).astype(BF16)
    start = nn(spread[0:16], before)
    start_hi = jnp.floor(start * (1.0 / 64.0))
    start_lo = start - 64.0 * start_hi
    row16 = iota((16, E), 0)
    tail = jnp.where(row16 == 0, start_hi, jnp.where(row16 == 1, start_lo, iota((16, E), 1).astype(F32)))
    ids = jnp.where(iota((SLOT, E), 0) < counts, blocks_ref[...], 2047)
    both = jnp.concatenate([lax.shift_right_logical(ids, 5), ids & 31], axis=0).astype(F32)
    table = jnp.concatenate([both, tail], axis=0).astype(BF16)
    lane = iota((1, CH), 1)
    sub = iota((SLOT, CH), 0).astype(F32)
    total = jnp.sum(granules).astype(I32)
    total_ref[0] = total

    def place(k, carry):
        pos = k * CH + lane
        gran = lax.shift_right_logical(pos, 3).astype(F32)
        hit = (first <= gran) & (gran < last)
        x = nn(table, jnp.where(hit, 1.0, 0.0).astype(BF16))
        slot = pos.astype(F32) - 8.0 * (64.0 * x[128:129] + x[129:130])
        code = 32.0 * x[0:64] + x[64:128]
        here = jnp.sum(jnp.where(sub == slot, code, 0.0), axis=0, keepdims=True).astype(I32)
        live = (pos < total * GR) & (here < B)
        ids_ref[k] = jnp.where(live, here, -1)
        ex_ref[k] = x[130:131].astype(I32)
        return carry

    chunks = lax.shift_right_logical(total + (GCH - 1), 5)
    lax.fori_loop(0, chunks, place, 0)

    hits = (iota((R, E), 0) == owner_ref[...]).astype(F32)
    earlier = nn(hits.astype(BF16), before)
    rank_ref[...] = jnp.sum(hits * earlier, axis=0, keepdims=True).astype(I32)

    def put(e, off):
        packed_ref[pl.ds(off, 8)] = values[pl.ds(e * 8, 8)]
        return off + lax.shift_right_logical(counts_s[e] + (GR - 1), 3)

    off = 0
    for i in range(LOADS):
        load(i).wait()
        off = lax.fori_loop(i * (E // LOADS), (i + 1) * (E // LOADS), put, off, unroll=8)
    packed_ref[pl.ds(off, GCH)] = jnp.zeros((GCH, GR, C), BF16)

    def send(k, carry):
        span = pl.ds(k * GCH, GCH)
        pltpu.make_async_copy(packed_ref.at[span], packed_hbm.at[span], out_sem).start()
        return carry

    lax.fori_loop(0, chunks, send, 0)
    whole = pl.ds(0, chunks * GCH)
    pltpu.make_async_copy(packed_ref.at[whole], packed_hbm.at[whole], out_sem).wait()


def start_chunks(packed_hbm, buf, sems, chunks):
    def go(k, carry):
        span = pl.ds(k * GCH, GCH)
        pltpu.make_async_copy(packed_hbm.at[span], buf.at[span], sems.at[k]).start()
        return carry

    lax.fori_loop(0, chunks, go, 0)


def wait_chunk(packed_hbm, buf, sems, k):
    span = pl.ds(k * GCH, GCH)
    pltpu.make_async_copy(packed_hbm.at[span], buf.at[span], sems.at[k]).wait()
    return buf[span].reshape(CH, C)


def margins_kernel(total_ref, w_ref, ids_ref, ex_ref, packed_hbm, out_ref, buf, acc, sems):
    chunks = lax.shift_right_logical(total_ref[0] + (GCH - 1), 5)
    start_chunks(packed_hbm, buf, sems, chunks)
    acc[...] = jnp.zeros_like(acc)
    rows = iota((E, CH), 0)
    sub8 = iota((8, CH), 0)

    def step(k, carry):
        v = wait_chunk(packed_hbm, buf, sems, k)
        ids = ids_ref[k]
        score = nt(w_ref[...], v)
        half = B // 2
        while half >= 8:
            bit = jnp.broadcast_to((ids & half) != 0, (half, CH))
            score = jnp.where(bit, score[half:], score[:half])
            half //= 2
        pick = jnp.sum(jnp.where(sub8 == (ids & 7), score, 0.0), axis=0, keepdims=True)
        pick = jnp.where(ids >= 0, pick, 0.0)
        acc[...] += jnp.where(rows == ex_ref[k], pick, 0.0)
        return carry

    lax.fori_loop(0, chunks, step, 0)
    row = jnp.sum(acc[...].T, axis=0, keepdims=True)
    out_ref[...] = jnp.broadcast_to(row[None], out_ref.shape)


def gradient_kernel(
    total_ref, parts_ref, labels_ref, owner_ref, rank_ref, ids_ref, ex_ref, packed_hbm, out_ref,
    buf, acc, sems
):
    chunks = lax.shift_right_logical(total_ref[0] + (GCH - 1), 5)
    start_chunks(packed_hbm, buf, sems, chunks)
    margin = jnp.sum(parts_ref[...].reshape(F, E), axis=0, keepdims=True)
    label = labels_ref[...].astype(F32)
    resid = jax.nn.sigmoid(margin) - label
    small = jnp.exp(-jnp.abs(margin))
    loss = jnp.sum(jnp.maximum(margin, 0.0) + jnp.log1p(small) - label * margin)
    half = resid.astype(BF16).astype(F32)
    column = jnp.broadcast_to(half, (C, E)).T
    column = jnp.concatenate([column, column], axis=1)
    rows = iota((E, CH), 0)
    lo_rows = iota((32, CH), 0)
    acc[...] = jnp.zeros_like(acc)

    def step(k, carry):
        v = wait_chunk(packed_hbm, buf, sems, k)
        ids = ids_ref[k]
        coef = jnp.sum(jnp.where(rows == ex_ref[k], column, 0.0), axis=0, keepdims=True)
        coef = jnp.where(ids >= 0, coef, 0.0)
        low = jnp.where(lo_rows == (ids & 31), coef, 0.0).astype(BF16)
        high = lax.shift_right_arithmetic(ids, 5)
        pieces = []
        for h in range(32):
            mask = jnp.broadcast_to(jnp.where(high == h, 1.0, 0.0), (32, CH)).astype(BF16)
            pieces.append(low * mask)
        spread = jnp.concatenate(pieces, axis=0)
        acc[...] += nn(spread, v)
        return carry

    lax.fori_loop(0, chunks, step, 0)
    out_ref[:, 0:32, :] = acc[...].reshape(R, 32, C).astype(BF16)

    owner_hit = iota((R, E), 0) == owner_ref[...]
    rank = rank_ref[...]
    lane_row = iota((C, E), 0)
    extra = jnp.zeros((R, C), F32)
    for i, piece in enumerate(split3(margin)):
        a = jnp.where(owner_hit, piece, 0.0).astype(BF16)
        b = jnp.where(lane_row == rank + OWN * i, 1.0, 0.0).astype(BF16)
        extra = extra + nt(a, b)
    lane = iota((R, C), 1)
    for i, piece in enumerate(split3(jnp.full((R, C), loss, F32))):
        extra = jnp.where(lane == 3 * OWN + i, piece, extra)
    out_ref[:, 32 : 32 + XR, :] = jnp.broadcast_to(extra[:, None, :], (R, XR, C)).astype(BF16)


def finish_kernel(in_ref, grad_ref, owned_ref, loss_ref):
    total = in_ref[0, 0:32, :].astype(F32)
    for r in range(1, R):
        total = total + in_ref[r, 0:32, :].astype(F32)
    grad_ref[...] = total
    extra = in_ref[:, 32 : 32 + XR, :].astype(F32)[:, 0, :]
    src = iota((C, E), 0)
    pick = jnp.where((src < 3 * OWN) & ((src & 7) == (iota((C, E), 1) & 7)), 1.0, 0.0)
    wide = nn(extra.astype(BF16), pick.astype(BF16))
    own = lax.shift_right_logical(iota((R, E), 1), 3) == iota((R, E), 0)
    owned_ref[...] = jnp.sum(jnp.where(own, wide, 0.0), axis=0, keepdims=True)
    lane = iota((R, C), 1)
    keep = (lane >= 3 * OWN) & (lane < 3 * OWN + 3)
    total_loss = jnp.sum(jnp.where(keep, extra, 0.0), keepdims=True)
    loss_ref[...] = total_loss * (1.0 / (E * R))


def local(body, out_shapes, in_specs, out_specs, scratch, limit, *args):
    return pl.pallas_call(
        body,
        out_shape=out_shapes,
        in_specs=in_specs,
        out_specs=out_specs,
        scratch_shapes=scratch,
        compiler_params=pltpu.CompilerParams(vmem_limit_bytes=limit << 20),
    )(*args)


def near(x):
    return pltpu.with_memory_space_constraint(x, pltpu.VMEM)


def far(x):
    return pltpu.with_memory_space_constraint(x, pltpu.HBM)


def on_device(tile_values, tile_blocks, tile_counts, labels, owner_rank, weights):
    shape = jax.ShapeDtypeStruct
    spread = local(
        spread_weights, pltpu.VMEM((R, B // R, C), BF16), [VMEM], VMEM, (), 8, weights
    )
    table = lax.all_to_all(spread, "rows", 0, 0, tiled=True).reshape(B, C)
    owner_row = owner_rank.reshape(1, E)
    label_row = labels.reshape(1, E)
    packed, ids, ex, rank, total = local(
        pack_tiles,
        (
            pltpu.HBM((NG, GR, C), BF16),
            pltpu.VMEM((NCH, 1, CH), I32),
            pltpu.VMEM((NCH, 1, CH), I32),
            pltpu.VMEM((1, E), I32),
            shape((1,), I32),
        ),
        [SMEM, VMEM, VMEM, VMEM, ANY],
        (ANY, VMEM, VMEM, VMEM, SMEM),
        [
            pltpu.VMEM((NG, GR, C), BF16),
            pltpu.VMEM((NG + GCH, GR, C), BF16),
            pltpu.SemaphoreType.DMA((LOADS,)),
            pltpu.SemaphoreType.DMA(()),
        ],
        20,
        tile_counts.reshape(E), tile_counts.T, tile_blocks.T, owner_row,
        far(tile_values.reshape(NG, GR, C)),
    )
    partial = local(
        margins_kernel, pltpu.VMEM((F, 1, E), F32), [SMEM, VMEM, VMEM, VMEM, ANY], VMEM,
        [pltpu.VMEM((NG, GR, C), BF16), pltpu.VMEM((E, CH), F32), pltpu.SemaphoreType.DMA((NCH,))], 16,
        total, near(table), near(ids), near(ex), far(packed),
    )
    parts = lax.all_to_all(partial, "feat", 0, 0, tiled=True)
    payload = local(
        gradient_kernel, pltpu.VMEM((R, B // R + XR, C), BF16),
        [SMEM, VMEM, VMEM, VMEM, VMEM, VMEM, VMEM, ANY], VMEM,
        [pltpu.VMEM((NG, GR, C), BF16), pltpu.VMEM((B, C), F32), pltpu.SemaphoreType.DMA((NCH,))], 16,
        total, near(parts), label_row, owner_row, near(rank), near(ids), near(ex), far(packed),
    )
    arrived = lax.all_to_all(payload, "rows", 0, 0, tiled=True)
    gradient, owned, loss = local(
        finish_kernel,
        (shape((B // R, C), F32), shape((1, E), F32), shape((1, 1), F32)),
        [VMEM], (VMEM, VMEM, VMEM), (), 8, near(arrived),
    )
    return owned.reshape(E), gradient, loss.reshape(())


def solution(mesh):
    in_specs = (
        P("rows", "feat", None),
        P("rows", "feat"),
        P("rows", "feat"),
        P("rows"),
        P("rows"),
        P(("feat", "rows"), None),
    )
    out_specs = (P("rows"), P(("feat", "rows"), None), P())
    return jax.shard_map(
        on_device, mesh=mesh, in_specs=in_specs, out_specs=out_specs, check_vma=False
    )
```

```python
import jax
import jax.numpy as jnp
from jax import lax
from jax.experimental import pallas as pl
from jax.experimental.pallas import tpu as pltpu
from jax.sharding import PartitionSpec as P

F32 = jnp.float32
BF16 = jnp.bfloat16
I32 = jnp.int32

E = 256
SLOT = 64
C = 128
B = 1024
R = 32
F = 8
OWN = 8
GR = 8
NG = E * SLOT // GR
CH = 512
GCH = CH // GR
NCH = NG // GCH
KA = 18
KAG = KA * GCH
LEAD = 2 * GCH
XR = 8
WIN = GCH + 8
LOADS = 4

VMEM = pl.BlockSpec(memory_space=pltpu.VMEM)
SMEM = pl.BlockSpec(memory_space=pltpu.SMEM)
ANY = pl.BlockSpec(memory_space=pl.ANY)


def nt(a, b):
    return lax.dot_general(a, b, (((1,), (1,)), ((), ())), preferred_element_type=F32)


def nn(a, b):
    return lax.dot_general(a, b, (((1,), (0,)), ((), ())), preferred_element_type=F32)


def split3(x):
    hi = x.astype(BF16).astype(F32)
    mid = (x - hi).astype(BF16).astype(F32)
    lo = (x - hi - mid).astype(BF16).astype(F32)
    return hi, mid, lo


def iota(shape, dim):
    return lax.broadcasted_iota(I32, shape, dim)


def spread_weights(w_hbm, out_ref, w_ref, sem):
    pltpu.make_async_copy(w_hbm, w_ref, sem).start()
    pltpu.make_async_copy(w_hbm, w_ref, sem).wait()
    out_ref[...] = jnp.broadcast_to(w_ref[...].astype(BF16)[None], out_ref.shape)


def pack_tiles(
    counts_s, counts_hbm, blocks_hbm, owner_hbm, values_hbm, near_ref, far_hbm, ids_ref, ex_ref,
    rank_ref, meta_ref, counts_ref, blocks_ref, owner_ref, values, spill, small_sems, sems, out_sem
):
    part = NG // LOADS
    small = [
        pltpu.make_async_copy(src, dst, small_sems.at[i])
        for i, (src, dst) in enumerate(
            [(counts_hbm, counts_ref), (blocks_hbm, blocks_ref), (owner_hbm, owner_ref)]
        )
    ]
    loads = [
        pltpu.make_async_copy(
            values_hbm.at[pl.ds(i * part, part)], values.at[pl.ds(i * part, part)], sems.at[i]
        )
        for i in range(LOADS)
    ]
    for copy in small + loads:
        copy.start()
    for copy in small:
        copy.wait()

    counts = counts_ref[...]
    granules = lax.shift_right_logical(counts + (GR - 1), 3).astype(F32)
    spread = jnp.broadcast_to(granules, (E, E)).astype(BF16)
    up = iota((E, E), 0)
    across = iota((E, E), 1)
    first = nt((across < up).astype(F32).astype(BF16), spread)
    last = nt((across <= up).astype(F32).astype(BF16), spread)
    first = jnp.concatenate([first] * (CH // E), axis=1)
    last = jnp.concatenate([last] * (CH // E), axis=1)
    before = (up < across).astype(F32).astype(BF16)
    start = nn(spread[0:16], before)
    start_hi = jnp.floor(start * (1.0 / 64.0))
    start_lo = start - 64.0 * start_hi
    row16 = iota((16, E), 0)
    tail = jnp.where(row16 == 0, start_hi, jnp.where(row16 == 1, start_lo, iota((16, E), 1).astype(F32)))
    ids = jnp.where(iota((SLOT, E), 0) < counts, blocks_ref[...], 2047)
    both = jnp.concatenate([lax.shift_right_logical(ids, 5), ids & 31], axis=0).astype(F32)
    table = jnp.concatenate([both, tail], axis=0).astype(BF16)
    lane = iota((1, CH), 1)
    sub = iota((SLOT, CH), 0).astype(F32)
    total = jnp.sum(granules).astype(I32)
    meta_ref[NCH + 1] = total
    meta_ref[0] = 0
    chunks = lax.shift_right_logical(total + (GCH - 1), 6)

    hits = (iota((R, E), 0) == owner_ref[...]).astype(F32)
    earlier = nn(hits.astype(BF16), before)
    rank_ref[...] = jnp.sum(hits * earlier, axis=0, keepdims=True).astype(I32)

    inside = jnp.sum(jnp.where(start[0:1] + 8.0 <= KAG, 1.0, 0.0)).astype(I32)
    reach = jnp.sum(jnp.where(start[0:1] < KAG, 1.0, 0.0)).astype(I32)
    blocks_inside = lax.shift_right_logical(inside, 3)

    def after(e, off):
        off = off + lax.shift_right_logical(counts_s[e] + (GR - 1), 3)
        meta_ref[lax.shift_right_logical(off + (GCH - 1), 6)] = e + 1
        return off

    def put_eight(i, off):
        for j in range(8):
            e = i * 8 + j
            near_ref[pl.ds(off, 8)] = values[pl.ds(e * 8, 8)]
            off = after(e, off)
        return off

    def put_both(e, off):
        tiles = values[pl.ds(e * 8, 8)]
        near_ref[pl.ds(off, 8)] = tiles
        spill[pl.ds(off - KAG + LEAD, 8)] = tiles
        return after(e, off)

    def put_far(e, off):
        spill[pl.ds(off - KAG + LEAD, 8)] = values[pl.ds(e * 8, 8)]
        return after(e, off)

    for copy in loads:
        copy.wait()
    off = lax.fori_loop(0, blocks_inside, put_eight, 0)
    off = lax.fori_loop(blocks_inside * 8, reach, put_both, off)
    lax.fori_loop(reach, E, put_far, off)
    zeros = jnp.zeros((GCH, GR, C), BF16)

    @pl.when(total <= KAG)
    def _():
        near_ref[pl.ds(total, GCH)] = zeros

    @pl.when(total > KAG)
    def _():
        spill[pl.ds(total - KAG + LEAD, GCH)] = zeros

    def send(k):
        return pltpu.make_async_copy(
            spill.at[pl.ds(LEAD + k * GCH, GCH)], far_hbm.at[pl.ds(k * GCH, GCH)], out_sem
        )

    def place(k, carry):
        pos = k * CH + lane
        gran = lax.shift_right_logical(pos, 3).astype(F32)
        hit = (first <= gran) & (gran < last)
        x = nn(table, jnp.where(hit, 1.0, 0.0).astype(BF16))
        slot = pos.astype(F32) - 8.0 * (64.0 * x[128:129] + x[129:130])
        code = 32.0 * x[0:64] + x[64:128]
        here = jnp.sum(jnp.where(sub == slot, code, 0.0), axis=0, keepdims=True).astype(I32)
        live = (pos < total * GR) & (here < B)
        ids_ref[k] = jnp.where(live, here, -1)
        ex_ref[k] = x[130:131].astype(I32)
        return carry

    lax.fori_loop(0, chunks, place, 0)

    def over(k, carry):
        send(k).start()
        send(k).wait()
        return carry

    lax.fori_loop(0, chunks - KA, over, 0)


def doubled(v, ids):
    top = jnp.broadcast_to(jnp.where(ids >= B // 2, 1.0, 0.0), (8, CH)).T
    mask = jnp.broadcast_to(top[:, 0:1], (CH, C)).astype(BF16)
    high = v * mask
    return v - high, high


def window(meta_ref, k):
    return pl.multiple_of(lax.shift_right_logical(meta_ref[k], 3) * 8, 8)


def margins_kernel(
    meta_ref, w_ref, ids_ref, ex_ref, near_ref, far_hbm, out_ref, buf, acc, wide, tiles0, tiles1,
    score0, score1, sem
):
    chunks = lax.shift_right_logical(meta_ref[NCH + 1] + (GCH - 1), 6)
    acc[...] = jnp.zeros_like(acc)
    wide[:, 0:C] = w_ref[0 : B // 2]
    wide[:, C : 2 * C] = w_ref[B // 2 : B]
    rows = iota((WIN, CH), 0)
    sub8 = iota((8, CH), 0)

    def prepare(k, tiles, source):
        low, high = doubled(source.reshape(CH, C), ids_ref[k])
        tiles[:, 0:C] = low
        tiles[:, C : 2 * C] = high

    def multiply(tiles, score):
        score[...] = nt(wide[...], tiles[...])

    def choose(k, score, live):
        ids = ids_ref[k]
        ids8 = jnp.broadcast_to(ids, (8, CH))
        pieces = [score[8 * i : 8 * i + 8, :] for i in range(B // 16)]
        half = B // 4
        while half >= 8:
            bit = (ids8 & half) != 0
            n = len(pieces) // 2
            pieces = [jnp.where(bit, pieces[n + i], pieces[i]) for i in range(n)]
            half //= 2
        pick = jnp.sum(jnp.where(sub8 == (ids8 & 7), pieces[0], 0.0), axis=0, keepdims=True)
        pick = jnp.where((ids >= 0) & live, pick, 0.0)
        base = window(meta_ref, k)
        span = pl.ds(base, WIN)
        acc[span, :] += jnp.where(rows + base == ex_ref[k], pick, 0.0)

    near = jnp.minimum(chunks, KA)
    final = near - 1

    def fetch(k):
        k = jnp.minimum(k, final)
        return k, near_ref[pl.ds(k * GCH, GCH)]

    k0, first = fetch(0)
    prepare(k0, tiles0, first)

    def pair(i, carry):
        k = 2 * i
        k1, v1 = fetch(k + 1)
        choose(jnp.clip(k - 1, 0, final), score1, (k >= 1) & (k <= near))
        multiply(tiles0, score0)
        prepare(k1, tiles1, v1)
        k2, v2 = fetch(k + 2)
        choose(jnp.minimum(k, final), score0, k < near)
        multiply(tiles1, score1)
        prepare(k2, tiles0, v2)
        return carry

    lax.fori_loop(0, lax.shift_right_logical(near + 2, 1), pair, 0)

    def outer(k, carry):
        copy = pltpu.make_async_copy(far_hbm.at[pl.ds((k - KA) * GCH, GCH)], buf, sem)
        copy.start()
        copy.wait()
        prepare(k, tiles0, buf[...])
        multiply(tiles0, score0)
        choose(k, score0, k < chunks)
        return carry

    lax.fori_loop(KA, chunks, outer, 0)
    row = jnp.sum(acc[0:E, :].T, axis=0, keepdims=True)
    out_ref[...] = jnp.broadcast_to(row[None], out_ref.shape)


def gradient_kernel(
    meta_ref, parts_ref, labels_hbm, owner_hbm, rank_ref, ids_ref, ex_ref, near_ref, far_hbm, out_ref,
    labels_ref, owner_ref, buf, acc, column_ref, tiles0, tiles1, hot0, hot1, small_sems, sem
):
    chunks = lax.shift_right_logical(meta_ref[NCH + 1] + (GCH - 1), 6)
    small = [
        pltpu.make_async_copy(labels_hbm, labels_ref, small_sems.at[0]),
        pltpu.make_async_copy(owner_hbm, owner_ref, small_sems.at[1]),
    ]
    for copy in small:
        copy.start()
    acc[...] = jnp.zeros_like(acc)
    margin = jnp.sum(parts_ref[...].reshape(F, E), axis=0, keepdims=True)
    small_exp = jnp.exp(-jnp.abs(margin))
    for copy in small:
        copy.wait()
    label = labels_ref[...].astype(F32)
    resid = jax.nn.sigmoid(margin) - label
    loss = jnp.sum(jnp.maximum(margin, 0.0) + jnp.log1p(small_exp) - label * margin)
    half = resid.astype(BF16).astype(F32)
    column_ref[0:E, :] = jnp.broadcast_to(half, (C, E)).T
    column_ref[E : E + WIN, :] = jnp.zeros((WIN, C), F32)
    rows = iota((WIN, CH), 0)
    lo_rows = iota((32, CH), 0)

    def prepare(k, tiles, hot, source, live):
        ids = ids_ref[k]
        base = window(meta_ref, k)
        column = column_ref[pl.ds(base, WIN), :]
        column = jnp.concatenate([column] * (CH // C), axis=1)
        coef = jnp.sum(jnp.where(rows + base == ex_ref[k], column, 0.0), axis=0, keepdims=True)
        coef = jnp.where((ids >= 0) & live, coef, 0.0)
        low = jnp.where(lo_rows == (ids & 31), coef, 0.0).astype(BF16)
        high = jnp.broadcast_to(lax.shift_right_arithmetic(ids, 5) & 15, (8, CH))
        for h in range(16):
            one = jnp.where(high == h, 1.0, 0.0)
            mask = jnp.concatenate([one, one, one, one], axis=0).astype(BF16)
            hot[32 * h : 32 * h + 32, :] = low * mask
        lower, upper = doubled(source.reshape(CH, C), ids)
        tiles[:, 0:C] = lower
        tiles[:, C : 2 * C] = upper

    def multiply(tiles, hot):
        acc[...] += nn(hot[...], tiles[...])

    near = jnp.minimum(chunks, KA)
    final = near - 1

    def fetch(k):
        live = k < near
        k = jnp.minimum(k, final)
        return k, near_ref[pl.ds(k * GCH, GCH)], live

    k0, v0, live0 = fetch(0)
    prepare(k0, tiles0, hot0, v0, live0)

    def pair(i, carry):
        k1, v1, live1 = fetch(2 * i + 1)
        multiply(tiles0, hot0)
        prepare(k1, tiles1, hot1, v1, live1)
        k2, v2, live2 = fetch(2 * i + 2)
        multiply(tiles1, hot1)
        prepare(k2, tiles0, hot0, v2, live2)
        return carry

    lax.fori_loop(0, lax.shift_right_logical(near + 1, 1), pair, 0)

    def outer(k, carry):
        copy = pltpu.make_async_copy(far_hbm.at[pl.ds((k - KA) * GCH, GCH)], buf, sem)
        copy.start()
        copy.wait()
        prepare(k, tiles0, hot0, buf[...], k < chunks)
        multiply(tiles0, hot0)
        return carry

    lax.fori_loop(KA, chunks, outer, 0)
    for i in range(2):
        out_ref[16 * i : 16 * i + 16, 0:32, :] = (
            acc[:, C * i : C * i + C].reshape(R // 2, 32, C).astype(BF16)
        )

    owner_hit = iota((R, E), 0) == owner_ref[...]
    rank = rank_ref[...]
    lane_row = iota((C, E), 0)
    extra = jnp.zeros((R, C), F32)
    for i, piece in enumerate(split3(margin)):
        a = jnp.where(owner_hit, piece, 0.0).astype(BF16)
        b = jnp.where(lane_row == rank + OWN * i, 1.0, 0.0).astype(BF16)
        extra = extra + nt(a, b)
    lane = iota((R, C), 1)
    for i, piece in enumerate(split3(jnp.full((R, C), loss, F32))):
        extra = jnp.where(lane == 3 * OWN + i, piece, extra)
    out_ref[:, 32 : 32 + XR, :] = jnp.broadcast_to(extra[:, None, :], (R, XR, C)).astype(BF16)


def finish_kernel(in_ref, grad_ref, owned_ref, loss_ref):
    total = in_ref[0, 0:32, :].astype(F32)
    for r in range(1, R):
        total = total + in_ref[r, 0:32, :].astype(F32)
    grad_ref[...] = total
    extra = in_ref[:, 32 : 32 + XR, :].astype(F32)[:, 0, :]
    src = iota((C, E), 0)
    pick = jnp.where((src < 3 * OWN) & ((src & 7) == (iota((C, E), 1) & 7)), 1.0, 0.0)
    wide = nn(extra.astype(BF16), pick.astype(BF16))
    own = lax.shift_right_logical(iota((R, E), 1), 3) == iota((R, E), 0)
    owned_ref[...] = jnp.sum(jnp.where(own, wide, 0.0), axis=0, keepdims=True)
    lane = iota((R, C), 1)
    keep = (lane >= 3 * OWN) & (lane < 3 * OWN + 3)
    total_loss = jnp.sum(jnp.where(keep, extra, 0.0), keepdims=True)
    loss_ref[...] = total_loss * (1.0 / (E * R))


def local(body, out_shapes, in_specs, out_specs, scratch, limit, *args):
    return pl.pallas_call(
        body,
        out_shape=out_shapes,
        in_specs=in_specs,
        out_specs=out_specs,
        scratch_shapes=scratch,
        compiler_params=pltpu.CompilerParams(vmem_limit_bytes=limit << 20),
    )(*args)


def near(x):
    return pltpu.with_memory_space_constraint(x, pltpu.VMEM)


def far(x):
    return pltpu.with_memory_space_constraint(x, pltpu.HBM)


def on_device(tile_values, tile_blocks, tile_counts, labels, owner_rank, weights):
    shape = jax.ShapeDtypeStruct
    dma = pltpu.SemaphoreType.DMA
    spread = local(
        spread_weights, pltpu.VMEM((R, B // R, C), BF16), [ANY], VMEM,
        [pltpu.VMEM((B // R, C), F32), dma(())], 4, far(weights),
    )
    table = lax.all_to_all(spread, "rows", 0, 0, tiled=True).reshape(B, C)
    owner_row = far(owner_rank.reshape(1, E))
    label_row = far(labels.reshape(1, E))
    packed, over, ids, ex, rank, meta = local(
        pack_tiles,
        (
            pltpu.VMEM((KAG + GCH, GR, C), BF16),
            pltpu.HBM((NG - KAG, GR, C), BF16),
            pltpu.VMEM((NCH, 1, CH), I32),
            pltpu.VMEM((NCH, 1, CH), I32),
            pltpu.VMEM((1, E), I32),
            shape((NCH + 2,), I32),
        ),
        [SMEM, ANY, ANY, ANY, ANY],
        (VMEM, ANY, VMEM, VMEM, VMEM, SMEM),
        [
            pltpu.VMEM((1, E), I32),
            pltpu.VMEM((SLOT, E), I32),
            pltpu.VMEM((1, E), I32),
            pltpu.VMEM((NG, GR, C), BF16),
            pltpu.VMEM((NG - KAG + LEAD + GCH, GR, C), BF16),
            dma((3,)),
            dma((LOADS,)),
            dma(()),
        ],
        16,
        tile_counts.reshape(E), far(tile_counts.T), far(tile_blocks.T), owner_row,
        far(tile_values.reshape(NG, GR, C)),
    )
    partial = local(
        margins_kernel, pltpu.VMEM((F, 1, E), F32), [SMEM, VMEM, VMEM, VMEM, VMEM, ANY], VMEM,
        [
            pltpu.VMEM((GCH, GR, C), BF16),
            pltpu.VMEM((E + WIN, CH), F32),
            pltpu.VMEM((B // 2, 2 * C), BF16),
            pltpu.VMEM((CH, 2 * C), BF16),
            pltpu.VMEM((CH, 2 * C), BF16),
            pltpu.VMEM((B // 2, CH), F32),
            pltpu.VMEM((B // 2, CH), F32),
            dma(()),
        ],
        16,
        meta, near(table), near(ids), near(ex), near(packed), far(over),
    )
    parts = lax.all_to_all(partial, "feat", 0, 0, tiled=True)
    payload = local(
        gradient_kernel, pltpu.VMEM((R, B // R + XR, C), BF16),
        [SMEM, VMEM, ANY, ANY, VMEM, VMEM, VMEM, VMEM, ANY], VMEM,
        [
            pltpu.VMEM((1, E), I32),
            pltpu.VMEM((1, E), I32),
            pltpu.VMEM((GCH, GR, C), BF16),
            pltpu.VMEM((B // 2, 2 * C), F32),
            pltpu.VMEM((E + WIN, C), F32),
            pltpu.VMEM((CH, 2 * C), BF16),
            pltpu.VMEM((CH, 2 * C), BF16),
            pltpu.VMEM((B // 2, CH), BF16),
            pltpu.VMEM((B // 2, CH), BF16),
            dma((2,)),
            dma(()),
        ],
        16,
        meta, near(parts), label_row, owner_row, near(rank), near(ids), near(ex), near(packed),
        far(over),
    )
    arrived = lax.all_to_all(payload, "rows", 0, 0, tiled=True)
    gradient, owned, loss = local(
        finish_kernel,
        (shape((B // R, C), F32), shape((1, E), F32), shape((1, 1), F32)),
        [VMEM], (VMEM, VMEM, VMEM), (), 8, near(arrived),
    )
    return owned.reshape(E), gradient, loss.reshape(())


def solution(mesh):
    in_specs = (
        P("rows", "feat", None),
        P("rows", "feat"),
        P("rows", "feat"),
        P("rows"),
        P("rows"),
        P(("feat", "rows"), None),
    )
    out_specs = (P("rows"), P(("feat", "rows"), None), P())
    return jax.shard_map(
        on_device, mesh=mesh, in_specs=in_specs, out_specs=out_specs, check_vma=False
    )
```

```python
import jax
import jax.numpy as jnp
from jax import lax
from jax.experimental import pallas as pl
from jax.experimental.pallas import tpu as pltpu
from jax.sharding import PartitionSpec as P

F32 = jnp.float32
BF16 = jnp.bfloat16
I32 = jnp.int32

E = 256
SLOT = 64
C = 128
B = 1024
R = 32
F = 8
OWN = 8
GR = 8
NG = E * SLOT // GR
CH = 512
GCH = CH // GR
NCH = NG // GCH
KA = 18
KAG = KA * GCH
LEAD = 2 * GCH
XR = 8
WIN = GCH + 8
FUSED = 4
LOADS = 4

VMEM = pl.BlockSpec(memory_space=pltpu.VMEM)
ANY = pl.BlockSpec(memory_space=pl.ANY)


def nt(a, b):
    return lax.dot_general(a, b, (((1,), (1,)), ((), ())), preferred_element_type=F32)


def nn(a, b):
    return lax.dot_general(a, b, (((1,), (0,)), ((), ())), preferred_element_type=F32)


def split3(x):
    hi = x.astype(BF16).astype(F32)
    mid = (x - hi).astype(BF16).astype(F32)
    lo = (x - hi - mid).astype(BF16).astype(F32)
    return hi, mid, lo


def iota(shape, dim):
    return lax.broadcasted_iota(I32, shape, dim)


def spread_weights(w_hbm, out_ref, w_ref, sem):
    pltpu.make_async_copy(w_hbm, w_ref, sem).start()
    pltpu.make_async_copy(w_hbm, w_ref, sem).wait()
    out_ref[...] = jnp.broadcast_to(w_ref[...].astype(BF16)[None], out_ref.shape)


def pack_tiles(
    flat_hbm, counts_hbm, blocks_hbm, owner_hbm, values_hbm, near_ref, far_hbm, ids_ref, ex_ref,
    info_ref, counts_s, counts_ref, blocks_ref, owner_ref, values, spill, small_sems, sems, out_sem
):
    part = NG // LOADS
    small = [
        pltpu.make_async_copy(src, dst, small_sems.at[i])
        for i, (src, dst) in enumerate(
            [
                (counts_hbm, counts_ref),
                (blocks_hbm, blocks_ref),
                (owner_hbm, owner_ref),
                (flat_hbm, counts_s),
            ]
        )
    ]
    loads = [
        pltpu.make_async_copy(
            values_hbm.at[pl.ds(i * part, part)], values.at[pl.ds(i * part, part)], sems.at[i]
        )
        for i in range(LOADS)
    ]
    for copy in small + loads:
        copy.start()
    for copy in small:
        copy.wait()

    counts = counts_ref[...]
    granules = lax.shift_right_logical(counts + (GR - 1), 3).astype(F32)
    spread = jnp.broadcast_to(granules, (E, E)).astype(BF16)
    up = iota((E, E), 0)
    across = iota((E, E), 1)
    first = nt((across < up).astype(F32).astype(BF16), spread)
    first = jnp.concatenate([first] * (CH // E), axis=1)
    before = (up < across).astype(F32).astype(BF16)
    start = nn(spread[0:16], before)
    start_hi = jnp.floor(start * (1.0 / 64.0))
    start_lo = start - 64.0 * start_hi
    row16 = iota((16, E), 0)
    tail = jnp.where(row16 == 0, start_hi, jnp.where(row16 == 1, start_lo, iota((16, E), 1).astype(F32)))
    ids = jnp.where(iota((SLOT, E), 0) < counts, blocks_ref[...], 2047)
    both = jnp.concatenate([lax.shift_right_logical(ids, 5), ids & 31], axis=0).astype(F32)
    table = jnp.concatenate([both, tail], axis=0)
    shifted = jnp.where(iota(table.shape, 1) == 0, 0.0, pltpu.roll(table, 1, 1))
    table = (table - shifted).astype(BF16)
    lane = iota((1, CH), 1)
    sub = iota((SLOT, CH), 0).astype(F32)
    total = jnp.sum(granules).astype(I32)
    chunks = lax.shift_right_logical(total + (GCH - 1), 6)

    hits = (iota((R, E), 0) == owner_ref[...]).astype(F32)
    earlier = nn(hits.astype(BF16), before)
    info_ref[0:1, :] = jnp.sum(hits * earlier, axis=0, keepdims=True).astype(I32)
    info_ref[1:2, :] = jnp.full((1, E), total, I32)

    def place(k, carry):
        pos = k * CH + lane
        gran = lax.shift_right_logical(pos, 3).astype(F32)
        x = nn(table, jnp.where(first <= gran, 1.0, 0.0).astype(BF16))
        slot = pos.astype(F32) - 8.0 * (64.0 * x[128:129] + x[129:130])
        code = 32.0 * x[0:64] + x[64:128]
        here = jnp.sum(jnp.where(sub == slot, code, 0.0), axis=0, keepdims=True).astype(I32)
        live = (pos < total * GR) & (here < B)
        ids_ref[k] = jnp.where(live, here, -1)
        ex_ref[k] = x[130:131].astype(I32)
        return carry


    inside = jnp.sum(jnp.where(start[0:1] + 8.0 <= KAG, 1.0, 0.0)).astype(I32)
    reach = jnp.sum(jnp.where(start[0:1] < KAG, 1.0, 0.0)).astype(I32)
    blocks_inside = lax.shift_right_logical(inside, 3)

    def after(e, off):
        return off + lax.shift_right_logical(counts_s[e] + (GR - 1), 3)

    def put_eight(i, off):
        for j in range(8):
            e = i * 8 + j
            near_ref[pl.ds(off, 8)] = values[pl.ds(e * 8, 8)]
            off = after(e, off)
        return off

    def put_both(e, off):
        tiles = values[pl.ds(e * 8, 8)]
        near_ref[pl.ds(off, 8)] = tiles
        spill[pl.ds(off - KAG + LEAD, 8)] = tiles
        return after(e, off)

    def put_far(e, off):
        spill[pl.ds(off - KAG + LEAD, 8)] = values[pl.ds(e * 8, 8)]
        return after(e, off)

    for copy in loads:
        copy.wait()

    def place_and_put(i, off):
        place(2 * i, 0)
        place(2 * i + 1, 0)
        for j in range(FUSED):
            off = put_eight(FUSED * i + j, off)
        return off

    @pl.when(inside == E)
    def _():
        lax.fori_loop(0, E // (8 * FUSED), place_and_put, 0)
        lax.fori_loop(2 * E // (8 * FUSED), chunks, place, 0)

    @pl.when(inside < E)
    def _():
        lax.fori_loop(0, chunks, place, 0)
        off = lax.fori_loop(0, blocks_inside, put_eight, 0)
        off = lax.fori_loop(blocks_inside * 8, reach, put_both, off)
        lax.fori_loop(reach, E, put_far, off)

    zeros = jnp.zeros((GCH, GR, C), BF16)

    @pl.when(total <= KAG)
    def _():
        near_ref[pl.ds(total, GCH)] = zeros

    @pl.when(total > KAG)
    def _():
        spill[pl.ds(total - KAG + LEAD, GCH)] = zeros

    def send(k):
        return pltpu.make_async_copy(
            spill.at[pl.ds(LEAD + k * GCH, GCH)], far_hbm.at[pl.ds(k * GCH, GCH)], out_sem
        )

    def over(k, carry):
        send(k).start()
        send(k).wait()
        return carry

    lax.fori_loop(0, chunks - KA, over, 0)


def doubled(v, ids):
    top = jnp.broadcast_to(jnp.where(ids >= B // 2, 1.0, 0.0), (8, CH)).T
    mask = jnp.broadcast_to(top[:, 0:1], (CH, C)).astype(BF16)
    high = v * mask
    return v - high, high


def scalar(row):
    return jnp.min(row[:, 0:128].astype(F32)).astype(I32)


def window(ex_ref, k):
    return pl.multiple_of(lax.shift_right_logical(scalar(ex_ref[k]), 3) * 8, 8)


def margins_kernel(
    info_ref, w_ref, ids_ref, ex_ref, near_ref, far_hbm, out_ref, buf, acc, wide, tiles0, tiles1, sem
):
    chunks = lax.shift_right_logical(scalar(info_ref[1:2, :]) + (GCH - 1), 6)
    acc[...] = jnp.zeros_like(acc)
    wide[:, 0:C] = w_ref[0 : B // 2]
    wide[:, C : 2 * C] = w_ref[B // 2 : B]
    rows = iota((WIN, CH), 0)
    sub8 = iota((8, CH), 0)

    def prepare(k, tiles, source):
        low, high = doubled(source.reshape(CH, C), ids_ref[k])
        tiles[:, 0:C] = low
        tiles[:, C : 2 * C] = high

    def multiply(tiles):
        return nt(wide[...], tiles[...])

    def choose(k, score, live):
        ids = ids_ref[k]
        ids8 = jnp.broadcast_to(ids, (8, CH))
        pieces = [score[8 * i : 8 * i + 8, :] for i in range(B // 16)]
        half = 8
        while len(pieces) > 1:
            bit = (ids8 & half) != 0
            pieces = [jnp.where(bit, b, a) for a, b in zip(pieces[0::2], pieces[1::2])]
            half *= 2
        pick = jnp.sum(jnp.where(sub8 == (ids8 & 7), pieces[0], 0.0), axis=0, keepdims=True)
        pick = jnp.where((ids >= 0) & live, pick, 0.0)
        base = window(ex_ref, k)
        span = pl.ds(base, WIN)
        acc[span, :] += jnp.where(rows + base == ex_ref[k], pick, 0.0)

    near = jnp.minimum(chunks, KA)
    final = near - 1

    def fetch(k):
        k = jnp.minimum(k, final)
        return k, near_ref[pl.ds(k * GCH, GCH)]

    k0, first = fetch(0)
    prepare(k0, tiles0, first)

    def pair(i, carry):
        k = 2 * i
        k1, v1 = fetch(k + 1)
        choose(k, multiply(tiles0), k < near)
        prepare(k1, tiles1, v1)
        k2, v2 = fetch(k + 2)
        choose(k1, multiply(tiles1), k + 1 < near)
        prepare(k2, tiles0, v2)
        return carry

    lax.fori_loop(0, lax.shift_right_logical(near + 1, 1), pair, 0)

    def outer(k, carry):
        copy = pltpu.make_async_copy(far_hbm.at[pl.ds((k - KA) * GCH, GCH)], buf, sem)
        copy.start()
        copy.wait()
        prepare(k, tiles0, buf[...])
        choose(k, multiply(tiles0), k < chunks)
        return carry

    lax.fori_loop(KA, chunks, outer, 0)
    row = jnp.sum(acc[0:E, :].T, axis=0, keepdims=True)
    out_ref[...] = jnp.broadcast_to(row[None], out_ref.shape)


def gradient_kernel(
    info_ref, parts_ref, labels_hbm, owner_hbm, ids_ref, ex_ref, near_ref, far_hbm, out_ref,
    labels_ref, owner_ref, buf, acc, column_ref, tiles0, tiles1, hot0, hot1, small_sems, sem
):
    chunks = lax.shift_right_logical(scalar(info_ref[1:2, :]) + (GCH - 1), 6)
    small = [
        pltpu.make_async_copy(labels_hbm, labels_ref, small_sems.at[0]),
        pltpu.make_async_copy(owner_hbm, owner_ref, small_sems.at[1]),
    ]
    for copy in small:
        copy.start()
    acc[...] = jnp.zeros_like(acc)
    margin = jnp.sum(parts_ref[...].reshape(F, E), axis=0, keepdims=True)
    small_exp = jnp.exp(-jnp.abs(margin))
    for copy in small:
        copy.wait()
    label = labels_ref[...].astype(F32)
    resid = jax.nn.sigmoid(margin) - label
    loss = jnp.sum(jnp.maximum(margin, 0.0) + jnp.log1p(small_exp) - label * margin)
    half = resid.astype(BF16).astype(F32)
    column_ref[0:E, :] = jnp.broadcast_to(half, (C, E)).T
    column_ref[E : E + WIN, :] = jnp.zeros((WIN, C), F32)
    rows = iota((WIN, CH), 0)
    lo_rows = iota((32, CH), 0)

    def prepare(k, tiles, hot, source, live):
        ids = ids_ref[k]
        base = window(ex_ref, k)
        column = column_ref[pl.ds(base, WIN), :]
        column = jnp.concatenate([column] * (CH // C), axis=1)
        coef = jnp.sum(jnp.where(rows + base == ex_ref[k], column, 0.0), axis=0, keepdims=True)
        coef = jnp.where((ids >= 0) & live, coef, 0.0)
        low = jnp.where(lo_rows == (ids & 31), coef, 0.0).astype(BF16)
        high = jnp.broadcast_to(lax.shift_right_arithmetic(ids, 5) & 15, (8, CH))
        for h in range(16):
            one = jnp.where(high == h, 1.0, 0.0)
            mask = jnp.concatenate([one, one, one, one], axis=0).astype(BF16)
            hot[32 * h : 32 * h + 32, :] = low * mask
        lower, upper = doubled(source.reshape(CH, C), ids)
        tiles[:, 0:C] = lower
        tiles[:, C : 2 * C] = upper

    def multiply(tiles, hot):
        acc[...] += nn(hot[...], tiles[...])

    near = jnp.minimum(chunks, KA)
    final = near - 1

    def fetch(k):
        live = k < near
        k = jnp.minimum(k, final)
        return k, near_ref[pl.ds(k * GCH, GCH)], live

    k0, v0, live0 = fetch(0)
    prepare(k0, tiles0, hot0, v0, live0)

    def pair(i, carry):
        k1, v1, live1 = fetch(2 * i + 1)
        multiply(tiles0, hot0)
        prepare(k1, tiles1, hot1, v1, live1)
        k2, v2, live2 = fetch(2 * i + 2)
        multiply(tiles1, hot1)
        prepare(k2, tiles0, hot0, v2, live2)
        return carry

    lax.fori_loop(0, lax.shift_right_logical(near + 1, 1), pair, 0)

    def outer(k, carry):
        copy = pltpu.make_async_copy(far_hbm.at[pl.ds((k - KA) * GCH, GCH)], buf, sem)
        copy.start()
        copy.wait()
        prepare(k, tiles0, hot0, buf[...], k < chunks)
        multiply(tiles0, hot0)
        return carry

    lax.fori_loop(KA, chunks, outer, 0)
    for i in range(2):
        out_ref[16 * i : 16 * i + 16, 0:32, :] = (
            acc[:, C * i : C * i + C].reshape(R // 2, 32, C).astype(BF16)
        )

    owner_hit = iota((R, E), 0) == owner_ref[...]
    rank = info_ref[0:1, :]
    lane_row = iota((C, E), 0)
    extra = jnp.zeros((R, C), F32)
    for i, piece in enumerate(split3(margin)):
        a = jnp.where(owner_hit, piece, 0.0).astype(BF16)
        b = jnp.where(lane_row == rank + OWN * i, 1.0, 0.0).astype(BF16)
        extra = extra + nt(a, b)
    lane = iota((R, C), 1)
    for i, piece in enumerate(split3(jnp.full((R, C), loss, F32))):
        extra = jnp.where(lane == 3 * OWN + i, piece, extra)
    out_ref[:, 32 : 32 + XR, :] = jnp.broadcast_to(extra[:, None, :], (R, XR, C)).astype(BF16)


def finish_kernel(in_ref, grad_ref, owned_ref, loss_ref):
    total = in_ref[0, 0:32, :].astype(F32)
    for r in range(1, R):
        total = total + in_ref[r, 0:32, :].astype(F32)
    grad_ref[...] = total
    extra = in_ref[:, 32 : 32 + XR, :].astype(F32)[:, 0, :]
    src = iota((C, E), 0)
    pick = jnp.where((src < 3 * OWN) & ((src & 7) == (iota((C, E), 1) & 7)), 1.0, 0.0)
    wide = nn(extra.astype(BF16), pick.astype(BF16))
    own = lax.shift_right_logical(iota((R, E), 1), 3) == iota((R, E), 0)
    owned_ref[...] = jnp.sum(jnp.where(own, wide, 0.0), axis=0, keepdims=True)
    lane = iota((R, C), 1)
    keep = (lane >= 3 * OWN) & (lane < 3 * OWN + 3)
    total_loss = jnp.sum(jnp.where(keep, extra, 0.0), keepdims=True)
    loss_ref[...] = total_loss * (1.0 / (E * R))


def local(body, out_shapes, in_specs, out_specs, scratch, limit, *args):
    return pl.pallas_call(
        body,
        out_shape=out_shapes,
        in_specs=in_specs,
        out_specs=out_specs,
        scratch_shapes=scratch,
        compiler_params=pltpu.CompilerParams(vmem_limit_bytes=limit << 20),
    )(*args)


def near(x):
    return pltpu.with_memory_space_constraint(x, pltpu.VMEM)


def far(x):
    return pltpu.with_memory_space_constraint(x, pltpu.HBM)


def on_device(tile_values, tile_blocks, tile_counts, labels, owner_rank, weights):
    shape = jax.ShapeDtypeStruct
    dma = pltpu.SemaphoreType.DMA
    spread = local(
        spread_weights, pltpu.VMEM((R, B // R, C), BF16), [ANY], VMEM,
        [pltpu.VMEM((B // R, C), F32), dma(())], 4, far(weights),
    )
    table = lax.all_to_all(spread, "rows", 0, 0, tiled=True).reshape(B, C)
    owner_row = far(owner_rank.reshape(1, E))
    label_row = far(labels.reshape(1, E))
    packed, over, ids, ex, info = local(
        pack_tiles,
        (
            pltpu.VMEM((KAG + GCH, GR, C), BF16),
            pltpu.HBM((NG - KAG, GR, C), BF16),
            pltpu.VMEM((NCH, 1, CH), I32),
            pltpu.VMEM((NCH, 1, CH), I32),
            pltpu.VMEM((2, E), I32),
        ),
        [ANY, ANY, ANY, ANY, ANY],
        (VMEM, ANY, VMEM, VMEM, VMEM),
        [
            pltpu.SMEM((E,), I32),
            pltpu.VMEM((1, E), I32),
            pltpu.VMEM((SLOT, E), I32),
            pltpu.VMEM((1, E), I32),
            pltpu.VMEM((NG, GR, C), BF16),
            pltpu.VMEM((NG - KAG + LEAD + GCH, GR, C), BF16),
            dma((4,)),
            dma((LOADS,)),
            dma(()),
        ],
        16,
        far(tile_counts.reshape(E)), far(tile_counts.T), far(tile_blocks.T), owner_row,
        far(tile_values.reshape(NG, GR, C)),
    )
    partial = local(
        margins_kernel, pltpu.VMEM((F, 1, E), F32), [VMEM, VMEM, VMEM, VMEM, VMEM, ANY], VMEM,
        [
            pltpu.VMEM((GCH, GR, C), BF16),
            pltpu.VMEM((E + WIN, CH), F32),
            pltpu.VMEM((B // 2, 2 * C), BF16),
            pltpu.VMEM((CH, 2 * C), BF16),
            pltpu.VMEM((CH, 2 * C), BF16),
            dma(()),
        ],
        16,
        near(info), near(table), near(ids), near(ex), near(packed), far(over),
    )
    parts = lax.all_to_all(partial, "feat", 0, 0, tiled=True)
    payload = local(
        gradient_kernel, pltpu.VMEM((R, B // R + XR, C), BF16),
        [VMEM, VMEM, ANY, ANY, VMEM, VMEM, VMEM, ANY], VMEM,
        [
            pltpu.VMEM((1, E), I32),
            pltpu.VMEM((1, E), I32),
            pltpu.VMEM((GCH, GR, C), BF16),
            pltpu.VMEM((B // 2, 2 * C), F32),
            pltpu.VMEM((E + WIN, C), F32),
            pltpu.VMEM((CH, 2 * C), BF16),
            pltpu.VMEM((CH, 2 * C), BF16),
            pltpu.VMEM((B // 2, CH), BF16),
            pltpu.VMEM((B // 2, CH), BF16),
            dma((2,)),
            dma(()),
        ],
        16,
        near(info), near(parts), label_row, owner_row, near(ids), near(ex), near(packed),
        far(over),
    )
    arrived = lax.all_to_all(payload, "rows", 0, 0, tiled=True)
    gradient, owned, loss = local(
        finish_kernel,
        (shape((B // R, C), F32), shape((1, E), F32), shape((1, 1), F32)),
        [VMEM], (VMEM, VMEM, VMEM), (), 8, near(arrived),
    )
    return owned.reshape(E), gradient, loss.reshape(())


def solution(mesh):
    in_specs = (
        P("rows", "feat", None),
        P("rows", "feat"),
        P("rows", "feat"),
        P("rows"),
        P("rows"),
        P(("feat", "rows"), None),
    )
    out_specs = (P("rows"), P(("feat", "rows"), None), P())
    return jax.shard_map(
        on_device, mesh=mesh, in_specs=in_specs, out_specs=out_specs, check_vma=False
    )
```

```python
import jax
import jax.numpy as jnp
from jax import lax
from jax.experimental import pallas as pl
from jax.experimental.pallas import tpu as pltpu
from jax.sharding import PartitionSpec as P

F32 = jnp.float32
BF16 = jnp.bfloat16
I32 = jnp.int32

E = 256
SLOT = 64
C = 128
B = 1024
R = 32
F = 8
OWN = 8
GR = 8
NG = E * SLOT // GR
CH = 512
GCH = CH // GR
NCH = NG // GCH
KA = 18
KAG = KA * GCH
LEAD = 2 * GCH
XR = 8
WIN = GCH + 8
FUSED = 4
LOADS = 4

VMEM = pl.BlockSpec(memory_space=pltpu.VMEM)
ANY = pl.BlockSpec(memory_space=pl.ANY)


def nt(a, b):
    return lax.dot_general(a, b, (((1,), (1,)), ((), ())), preferred_element_type=F32)


def nn(a, b):
    return lax.dot_general(a, b, (((1,), (0,)), ((), ())), preferred_element_type=F32)


def split3(x):
    hi = x.astype(BF16).astype(F32)
    mid = (x - hi).astype(BF16).astype(F32)
    lo = (x - hi - mid).astype(BF16).astype(F32)
    return hi, mid, lo


def iota(shape, dim):
    return lax.broadcasted_iota(I32, shape, dim)


def spread_weights(w_hbm, out_ref, w_ref, sem):
    pltpu.make_async_copy(w_hbm, w_ref, sem).start()
    pltpu.make_async_copy(w_hbm, w_ref, sem).wait()
    out_ref[...] = jnp.broadcast_to(w_ref[...].astype(BF16)[None], out_ref.shape)


def pack_tiles(
    flat_hbm, counts_hbm, blocks_hbm, owner_hbm, labels_hbm, values_hbm, near_ref, far_hbm, ids_ref, ex_ref,
    info_ref, counts_s, counts_ref, blocks_ref, owner_ref, labels_ref, values, spill, small_sems, sems, out_sem
):
    part = NG // LOADS
    small = [
        pltpu.make_async_copy(src, dst, small_sems.at[i])
        for i, (src, dst) in enumerate(
            [
                (counts_hbm, counts_ref),
                (blocks_hbm, blocks_ref),
                (owner_hbm, owner_ref),
                (flat_hbm, counts_s),
                (labels_hbm, labels_ref),
            ]
        )
    ]
    loads = [
        pltpu.make_async_copy(
            values_hbm.at[pl.ds(i * part, part)], values.at[pl.ds(i * part, part)], sems.at[i]
        )
        for i in range(LOADS)
    ]
    for copy in small + loads:
        copy.start()
    for copy in small:
        copy.wait()

    counts = counts_ref[...]
    granules = lax.shift_right_logical(counts + (GR - 1), 3).astype(F32)
    spread = jnp.broadcast_to(granules, (E, E)).astype(BF16)
    up = iota((E, E), 0)
    across = iota((E, E), 1)
    first = nt((across < up).astype(F32).astype(BF16), spread)
    first = jnp.concatenate([first] * (CH // E), axis=1)
    before = (up < across).astype(F32).astype(BF16)
    start = nn(spread[0:16], before)
    start_hi = jnp.floor(start * (1.0 / 64.0))
    start_lo = start - 64.0 * start_hi
    row16 = iota((16, E), 0)
    tail = jnp.where(row16 == 0, start_hi, jnp.where(row16 == 1, start_lo, iota((16, E), 1).astype(F32)))
    ids = jnp.where(iota((SLOT, E), 0) < counts, blocks_ref[...], 2047)
    both = jnp.concatenate([lax.shift_right_logical(ids, 5), ids & 31], axis=0).astype(F32)
    table = jnp.concatenate([both, tail], axis=0)
    shifted = jnp.where(iota(table.shape, 1) == 0, 0.0, pltpu.roll(table, 1, 1))
    table = (table - shifted).astype(BF16)
    lane = iota((1, CH), 1)
    sub = iota((SLOT, CH), 0).astype(F32)
    total = jnp.sum(granules).astype(I32)
    chunks = lax.shift_right_logical(total + (GCH - 1), 6)

    hits = (iota((R, E), 0) == owner_ref[...]).astype(F32)
    earlier = nn(hits.astype(BF16), before)
    info_ref[0:1, :] = jnp.sum(hits * earlier, axis=0, keepdims=True).astype(I32)
    info_ref[1:2, :] = jnp.full((1, E), total, I32)
    info_ref[2:3, :] = owner_ref[...]
    info_ref[3:4, :] = labels_ref[...]

    def place(k, carry):
        pos = k * CH + lane
        gran = lax.shift_right_logical(pos, 3).astype(F32)
        x = nn(table, jnp.where(first <= gran, 1.0, 0.0).astype(BF16))
        slot = pos.astype(F32) - 8.0 * (64.0 * x[128:129] + x[129:130])
        code = 32.0 * x[0:64] + x[64:128]
        here = jnp.sum(jnp.where(sub == slot, code, 0.0), axis=0, keepdims=True).astype(I32)
        live = (pos < total * GR) & (here < B)
        ids_ref[k] = jnp.where(live, here, -1)
        ex_ref[k] = x[130:131].astype(I32)
        return carry


    inside = jnp.sum(jnp.where(start[0:1] + 8.0 <= KAG, 1.0, 0.0)).astype(I32)
    reach = jnp.sum(jnp.where(start[0:1] < KAG, 1.0, 0.0)).astype(I32)
    blocks_inside = lax.shift_right_logical(inside, 3)

    def after(e, off):
        return off + lax.shift_right_logical(counts_s[e] + (GR - 1), 3)

    def put_eight(i, off):
        for j in range(8):
            e = i * 8 + j
            near_ref[pl.ds(off, 8)] = values[pl.ds(e * 8, 8)]
            off = after(e, off)
        return off

    def put_both(e, off):
        tiles = values[pl.ds(e * 8, 8)]
        near_ref[pl.ds(off, 8)] = tiles
        spill[pl.ds(off - KAG + LEAD, 8)] = tiles
        return after(e, off)

    def put_far(e, off):
        spill[pl.ds(off - KAG + LEAD, 8)] = values[pl.ds(e * 8, 8)]
        return after(e, off)

    for copy in loads:
        copy.wait()

    def place_and_put(i, off):
        place(2 * i, 0)
        place(2 * i + 1, 0)
        for j in range(FUSED):
            off = put_eight(FUSED * i + j, off)
        return off

    @pl.when(inside == E)
    def _():
        lax.fori_loop(0, E // (8 * FUSED), place_and_put, 0)
        lax.fori_loop(2 * E // (8 * FUSED), chunks, place, 0)

    @pl.when(inside < E)
    def _():
        lax.fori_loop(0, chunks, place, 0)
        off = lax.fori_loop(0, blocks_inside, put_eight, 0)
        off = lax.fori_loop(blocks_inside * 8, reach, put_both, off)
        lax.fori_loop(reach, E, put_far, off)

    zeros = jnp.zeros((GCH, GR, C), BF16)

    @pl.when(total <= KAG)
    def _():
        near_ref[pl.ds(total, GCH)] = zeros

    @pl.when(total > KAG)
    def _():
        spill[pl.ds(total - KAG + LEAD, GCH)] = zeros

    def send(k):
        return pltpu.make_async_copy(
            spill.at[pl.ds(LEAD + k * GCH, GCH)], far_hbm.at[pl.ds(k * GCH, GCH)], out_sem
        )

    def over(k, carry):
        send(k).start()
        send(k).wait()
        return carry

    lax.fori_loop(0, chunks - KA, over, 0)


def doubled(v, ids):
    top = jnp.broadcast_to(jnp.where(ids >= B // 2, 1.0, 0.0), (8, CH)).T
    mask = jnp.broadcast_to(top[:, 0:1], (CH, C)).astype(BF16)
    high = v * mask
    return v - high, high


def scalar(row):
    return jnp.min(row[:, 0:128].astype(F32)).astype(I32)


def window(ex_ref, k):
    return pl.multiple_of(lax.shift_right_logical(scalar(ex_ref[k]), 3) * 8, 8)


def margins_kernel(
    info_ref, w_ref, ids_ref, ex_ref, near_ref, far_hbm, out_ref, buf, acc, wide, tiles0, tiles1, sem
):
    chunks = lax.shift_right_logical(scalar(info_ref[1:2, :]) + (GCH - 1), 6)
    acc[...] = jnp.zeros_like(acc)
    wide[:, 0:C] = w_ref[0 : B // 2]
    wide[:, C : 2 * C] = w_ref[B // 2 : B]
    rows = iota((WIN, CH), 0)
    sub8 = iota((8, CH), 0)

    def prepare(k, tiles, source):
        low, high = doubled(source.reshape(CH, C), ids_ref[k])
        tiles[:, 0:C] = low
        tiles[:, C : 2 * C] = high

    def multiply(tiles):
        return nt(wide[...], tiles[...])

    def choose(k, score, live):
        ids = ids_ref[k]
        ids8 = jnp.broadcast_to(ids, (8, CH))
        pieces = [score[8 * i : 8 * i + 8, :] for i in range(B // 16)]
        half = 8
        while len(pieces) > 1:
            bit = (ids8 & half) != 0
            pieces = [jnp.where(bit, b, a) for a, b in zip(pieces[0::2], pieces[1::2])]
            half *= 2
        pick = jnp.sum(jnp.where(sub8 == (ids8 & 7), pieces[0], 0.0), axis=0, keepdims=True)
        pick = jnp.where((ids >= 0) & live, pick, 0.0)
        base = window(ex_ref, k)
        span = pl.ds(base, WIN)
        acc[span, :] += jnp.where(rows + base == ex_ref[k], pick, 0.0)

    near = jnp.minimum(chunks, KA)
    final = near - 1

    def fetch(k):
        k = jnp.minimum(k, final)
        return k, near_ref[pl.ds(k * GCH, GCH)]

    def ahead(k):
        for tiles, j in ((tiles0, k), (tiles1, k + 1)):
            j, v = fetch(j)
            prepare(j, tiles, v)

    ahead(0)

    def pair(i, carry):
        k = 2 * i
        choose(k, multiply(tiles0), k < near)
        choose(jnp.minimum(k + 1, final), multiply(tiles1), k + 1 < near)
        ahead(k + 2)
        return carry

    lax.fori_loop(0, lax.shift_right_logical(near + 1, 1), pair, 0)

    def outer(k, carry):
        copy = pltpu.make_async_copy(far_hbm.at[pl.ds((k - KA) * GCH, GCH)], buf, sem)
        copy.start()
        copy.wait()
        prepare(k, tiles0, buf[...])
        choose(k, multiply(tiles0), k < chunks)
        return carry

    lax.fori_loop(KA, chunks, outer, 0)
    row = jnp.sum(acc[0:E, :].T, axis=0, keepdims=True)
    out_ref[...] = jnp.broadcast_to(row[None], out_ref.shape)


def gradient_kernel(
    info_ref, parts_ref, ids_ref, ex_ref, near_ref, far_hbm, out_ref, buf, acc, column_ref,
    tiles0, tiles1, hot0, hot1, sem
):
    chunks = lax.shift_right_logical(scalar(info_ref[1:2, :]) + (GCH - 1), 6)
    acc[...] = jnp.zeros_like(acc)
    margin = jnp.sum(parts_ref[...].reshape(F, E), axis=0, keepdims=True)
    small_exp = jnp.exp(-jnp.abs(margin))
    label = info_ref[3:4, :].astype(F32)
    resid = jax.nn.sigmoid(margin) - label
    loss = jnp.sum(jnp.maximum(margin, 0.0) + jnp.log1p(small_exp) - label * margin)
    half = resid.astype(BF16).astype(F32)
    column_ref[0:E, :] = jnp.broadcast_to(half, (C, E)).T
    column_ref[E : E + WIN, :] = jnp.zeros((WIN, C), F32)
    rows = iota((WIN, CH), 0)
    lo_rows = iota((32, CH), 0)

    def prepare(k, tiles, hot, source, live):
        ids = ids_ref[k]
        base = window(ex_ref, k)
        column = column_ref[pl.ds(base, WIN), :]
        column = jnp.concatenate([column] * (CH // C), axis=1)
        coef = jnp.sum(jnp.where(rows + base == ex_ref[k], column, 0.0), axis=0, keepdims=True)
        coef = jnp.where((ids >= 0) & live, coef, 0.0)
        low = jnp.where(lo_rows == (ids & 31), coef, 0.0).astype(BF16)
        high = jnp.broadcast_to(lax.shift_right_arithmetic(ids, 5) & 15, (8, CH))
        for h in range(16):
            one = jnp.where(high == h, 1.0, 0.0)
            mask = jnp.concatenate([one, one, one, one], axis=0).astype(BF16)
            hot[32 * h : 32 * h + 32, :] = low * mask
        lower, upper = doubled(source.reshape(CH, C), ids)
        tiles[:, 0:C] = lower
        tiles[:, C : 2 * C] = upper

    def multiply(tiles, hot):
        acc[...] += nn(hot[...], tiles[...])

    near = jnp.minimum(chunks, KA)
    final = near - 1

    def fetch(k):
        live = k < near
        k = jnp.minimum(k, final)
        return k, near_ref[pl.ds(k * GCH, GCH)], live

    def ahead(k):
        for tiles, hot, j in ((tiles0, hot0, k), (tiles1, hot1, k + 1)):
            j, v, live = fetch(j)
            prepare(j, tiles, hot, v, live)

    ahead(0)

    def pair(i, carry):
        acc[...] += nn(hot0[...], tiles0[...]) + nn(hot1[...], tiles1[...])
        ahead(2 * i + 2)
        return carry

    lax.fori_loop(0, lax.shift_right_logical(near + 1, 1), pair, 0)

    def outer(k, carry):
        copy = pltpu.make_async_copy(far_hbm.at[pl.ds((k - KA) * GCH, GCH)], buf, sem)
        copy.start()
        copy.wait()
        prepare(k, tiles0, hot0, buf[...], k < chunks)
        multiply(tiles0, hot0)
        return carry

    lax.fori_loop(KA, chunks, outer, 0)
    for i in range(2):
        out_ref[16 * i : 16 * i + 16, 0:32, :] = (
            acc[:, C * i : C * i + C].reshape(R // 2, 32, C).astype(BF16)
        )

    owner_hit = iota((R, E), 0) == info_ref[2:3, :]
    rank = info_ref[0:1, :]
    lane_row = iota((C, E), 0)
    extra = jnp.zeros((R, C), F32)
    for i, piece in enumerate(split3(margin)):
        a = jnp.where(owner_hit, piece, 0.0).astype(BF16)
        b = jnp.where(lane_row == rank + OWN * i, 1.0, 0.0).astype(BF16)
        extra = extra + nt(a, b)
    lane = iota((R, C), 1)
    for i, piece in enumerate(split3(jnp.full((R, C), loss, F32))):
        extra = jnp.where(lane == 3 * OWN + i, piece, extra)
    out_ref[:, 32 : 32 + XR, :] = jnp.broadcast_to(extra[:, None, :], (R, XR, C)).astype(BF16)


def finish_kernel(in_ref, grad_ref, owned_ref, loss_ref):
    total = in_ref[0, 0:32, :].astype(F32)
    for r in range(1, R):
        total = total + in_ref[r, 0:32, :].astype(F32)
    grad_ref[...] = total
    extra = in_ref[:, 32 : 32 + XR, :].astype(F32)[:, 0, :]
    src = iota((C, E), 0)
    pick = jnp.where((src < 3 * OWN) & ((src & 7) == (iota((C, E), 1) & 7)), 1.0, 0.0)
    wide = nn(extra.astype(BF16), pick.astype(BF16))
    own = lax.shift_right_logical(iota((R, E), 1), 3) == iota((R, E), 0)
    owned_ref[...] = jnp.sum(jnp.where(own, wide, 0.0), axis=0, keepdims=True)
    lane = iota((R, C), 1)
    keep = (lane >= 3 * OWN) & (lane < 3 * OWN + 3)
    total_loss = jnp.sum(jnp.where(keep, extra, 0.0), keepdims=True)
    loss_ref[...] = total_loss * (1.0 / (E * R))


def local(body, out_shapes, in_specs, out_specs, scratch, limit, *args):
    return pl.pallas_call(
        body,
        out_shape=out_shapes,
        in_specs=in_specs,
        out_specs=out_specs,
        scratch_shapes=scratch,
        compiler_params=pltpu.CompilerParams(vmem_limit_bytes=limit << 20),
    )(*args)


def near(x):
    return pltpu.with_memory_space_constraint(x, pltpu.VMEM)


def far(x):
    return pltpu.with_memory_space_constraint(x, pltpu.HBM)


def on_device(tile_values, tile_blocks, tile_counts, labels, owner_rank, weights):
    shape = jax.ShapeDtypeStruct
    dma = pltpu.SemaphoreType.DMA
    spread = local(
        spread_weights, pltpu.VMEM((R, B // R, C), BF16), [ANY], VMEM,
        [pltpu.VMEM((B // R, C), F32), dma(())], 4, far(weights),
    )
    table = lax.all_to_all(spread, "rows", 0, 0, tiled=True).reshape(B, C)
    owner_row = far(owner_rank.reshape(1, E))
    label_row = far(labels.reshape(1, E))
    packed, over, ids, ex, info = local(
        pack_tiles,
        (
            pltpu.VMEM((KAG + GCH, GR, C), BF16),
            pltpu.HBM((NG - KAG, GR, C), BF16),
            pltpu.VMEM((NCH, 1, CH), I32),
            pltpu.VMEM((NCH, 1, CH), I32),
            pltpu.VMEM((4, E), I32),
        ),
        [ANY, ANY, ANY, ANY, ANY, ANY],
        (VMEM, ANY, VMEM, VMEM, VMEM),
        [
            pltpu.SMEM((E,), I32),
            pltpu.VMEM((1, E), I32),
            pltpu.VMEM((SLOT, E), I32),
            pltpu.VMEM((1, E), I32),
            pltpu.VMEM((1, E), I32),
            pltpu.VMEM((NG, GR, C), BF16),
            pltpu.VMEM((NG - KAG + LEAD + GCH, GR, C), BF16),
            dma((5,)),
            dma((LOADS,)),
            dma(()),
        ],
        16,
        far(tile_counts.reshape(E)), far(tile_counts.T), far(tile_blocks.T), owner_row, label_row,
        far(tile_values.reshape(NG, GR, C)),
    )
    partial = local(
        margins_kernel, pltpu.VMEM((F, 1, E), F32), [VMEM, VMEM, VMEM, VMEM, VMEM, ANY], VMEM,
        [
            pltpu.VMEM((GCH, GR, C), BF16),
            pltpu.VMEM((E + WIN, CH), F32),
            pltpu.VMEM((B // 2, 2 * C), BF16),
            pltpu.VMEM((CH, 2 * C), BF16),
            pltpu.VMEM((CH, 2 * C), BF16),
            dma(()),
        ],
        16,
        near(info), near(table), near(ids), near(ex), near(packed), far(over),
    )
    parts = lax.all_to_all(partial, "feat", 0, 0, tiled=True)
    payload = local(
        gradient_kernel, pltpu.VMEM((R, B // R + XR, C), BF16),
        [VMEM, VMEM, VMEM, VMEM, VMEM, ANY], VMEM,
        [
            pltpu.VMEM((GCH, GR, C), BF16),
            pltpu.VMEM((B // 2, 2 * C), F32),
            pltpu.VMEM((E + WIN, C), F32),
            pltpu.VMEM((CH, 2 * C), BF16),
            pltpu.VMEM((CH, 2 * C), BF16),
            pltpu.VMEM((B // 2, CH), BF16),
            pltpu.VMEM((B // 2, CH), BF16),
            dma(()),
        ],
        16,
        near(info), near(parts), near(ids), near(ex), near(packed),
        far(over),
    )
    arrived = lax.all_to_all(payload, "rows", 0, 0, tiled=True)
    gradient, owned, loss = local(
        finish_kernel,
        (shape((B // R, C), F32), shape((1, E), F32), shape((1, 1), F32)),
        [VMEM], (VMEM, VMEM, VMEM), (), 8, near(arrived),
    )
    return owned.reshape(E), gradient, loss.reshape(())


def solution(mesh):
    in_specs = (
        P("rows", "feat", None),
        P("rows", "feat"),
        P("rows", "feat"),
        P("rows"),
        P("rows"),
        P(("feat", "rows"), None),
    )
    out_specs = (P("rows"), P(("feat", "rows"), None), P())
    return jax.shard_map(
        on_device, mesh=mesh, in_specs=in_specs, out_specs=out_specs, check_vma=False
    )
```

```python
import jax
import jax.numpy as jnp
from jax import lax
from jax.experimental import pallas as pl
from jax.experimental.pallas import tpu as pltpu
from jax.sharding import PartitionSpec as P

F32 = jnp.float32
BF16 = jnp.bfloat16
I32 = jnp.int32

E = 256
SLOT = 64
C = 128
B = 1024
R = 32
F = 8
OWN = 8
GR = 8
NG = E * SLOT // GR
CH = 512
GCH = CH // GR
NCH = NG // GCH
KA = 18
KAG = KA * GCH
LEAD = 2 * GCH
XR = 8
WIN = GCH + 8
FUSED = 4
LOADS = 4

VMEM = pl.BlockSpec(memory_space=pltpu.VMEM)
ANY = pl.BlockSpec(memory_space=pl.ANY)


def nt(a, b):
    return lax.dot_general(a, b, (((1,), (1,)), ((), ())), preferred_element_type=F32)


def nn(a, b):
    return lax.dot_general(a, b, (((1,), (0,)), ((), ())), preferred_element_type=F32)


def split3(x):
    hi = x.astype(BF16).astype(F32)
    mid = (x - hi).astype(BF16).astype(F32)
    lo = (x - hi - mid).astype(BF16).astype(F32)
    return hi, mid, lo


def iota(shape, dim):
    return lax.broadcasted_iota(I32, shape, dim)


def spread_weights(w_hbm, out_ref, w_ref, sem):
    pltpu.make_async_copy(w_hbm, w_ref, sem).start()
    pltpu.make_async_copy(w_hbm, w_ref, sem).wait()
    out_ref[...] = jnp.broadcast_to(w_ref[...].astype(BF16)[None], out_ref.shape)


def pack_tiles(
    flat_hbm, counts_hbm, blocks_hbm, owner_hbm, labels_hbm, values_hbm, near_ref, far_hbm, ids_ref, ex_ref,
    info_ref, counts_s, counts_ref, blocks_ref, owner_ref, labels_ref, values, spill, small_sems, sems, out_sem
):
    part = NG // LOADS
    small = [
        pltpu.make_async_copy(src, dst, small_sems.at[i])
        for i, (src, dst) in enumerate(
            [
                (counts_hbm, counts_ref),
                (blocks_hbm, blocks_ref),
                (owner_hbm, owner_ref),
                (flat_hbm, counts_s),
                (labels_hbm, labels_ref),
            ]
        )
    ]
    loads = [
        pltpu.make_async_copy(
            values_hbm.at[pl.ds(i * part, part)], values.at[pl.ds(i * part, part)], sems.at[i]
        )
        for i in range(LOADS)
    ]
    for copy in small + loads:
        copy.start()
    for copy in small:
        copy.wait()

    counts = counts_ref[...]
    granules = lax.shift_right_logical(counts + (GR - 1), 3).astype(F32)
    spread = jnp.broadcast_to(granules, (E, E)).astype(BF16)
    up = iota((E, E), 0)
    across = iota((E, E), 1)
    first = nt((across < up).astype(F32).astype(BF16), spread)
    first = jnp.concatenate([first] * (CH // E), axis=1)
    before = (up < across).astype(F32).astype(BF16)
    start = nn(spread[0:16], before)
    start_hi = jnp.floor(start * (1.0 / 64.0))
    start_lo = start - 64.0 * start_hi
    row16 = iota((16, E), 0)
    tail = jnp.where(row16 == 0, start_hi, jnp.where(row16 == 1, start_lo, iota((16, E), 1).astype(F32)))
    ids = jnp.where(iota((SLOT, E), 0) < counts, blocks_ref[...], 2047)
    both = jnp.concatenate([lax.shift_right_logical(ids, 5), ids & 31], axis=0).astype(F32)
    table = jnp.concatenate([both, tail], axis=0)
    shifted = jnp.where(iota(table.shape, 1) == 0, 0.0, pltpu.roll(table, 1, 1))
    table = (table - shifted).astype(BF16)
    lane = iota((1, CH), 1)
    sub = iota((SLOT, CH), 0).astype(F32)
    total = jnp.sum(granules).astype(I32)
    chunks = lax.shift_right_logical(total + (GCH - 1), 6)

    hits = (iota((R, E), 0) == owner_ref[...]).astype(F32)
    earlier = nn(hits.astype(BF16), before)
    info_ref[0:1, :] = jnp.sum(hits * earlier, axis=0, keepdims=True).astype(I32)
    info_ref[1:2, :] = jnp.full((1, E), total, I32)
    info_ref[2:3, :] = owner_ref[...]
    info_ref[3:4, :] = labels_ref[...]

    def place(k, carry):
        pos = k * CH + lane
        gran = lax.shift_right_logical(pos, 3).astype(F32)
        x = nn(table, jnp.where(first <= gran, 1.0, 0.0).astype(BF16))
        slot = pos.astype(F32) - 8.0 * (64.0 * x[128:129] + x[129:130])
        code = 32.0 * x[0:64] + x[64:128]
        here = jnp.sum(jnp.where(sub == slot, code, 0.0), axis=0, keepdims=True).astype(I32)
        live = (pos < total * GR) & (here < B)
        ids_ref[k] = jnp.where(live, here, -1)
        ex_ref[k] = x[130:131].astype(I32)
        return carry


    inside = jnp.sum(jnp.where(start[0:1] + 8.0 <= KAG, 1.0, 0.0)).astype(I32)
    reach = jnp.sum(jnp.where(start[0:1] < KAG, 1.0, 0.0)).astype(I32)
    blocks_inside = lax.shift_right_logical(inside, 3)

    def after(e, off):
        return off + lax.shift_right_logical(counts_s[e] + (GR - 1), 3)

    def put_eight(i, off):
        for j in range(8):
            e = i * 8 + j
            near_ref[pl.ds(off, 8)] = values[pl.ds(e * 8, 8)]
            off = after(e, off)
        return off

    def put_both(e, off):
        tiles = values[pl.ds(e * 8, 8)]
        near_ref[pl.ds(off, 8)] = tiles
        spill[pl.ds(off - KAG + LEAD, 8)] = tiles
        return after(e, off)

    def put_far(e, off):
        spill[pl.ds(off - KAG + LEAD, 8)] = values[pl.ds(e * 8, 8)]
        return after(e, off)

    for copy in loads:
        copy.wait()

    def place_and_put(i, off):
        place(2 * i, 0)
        place(2 * i + 1, 0)
        for j in range(FUSED):
            off = put_eight(FUSED * i + j, off)
        return off

    @pl.when(inside == E)
    def _():
        lax.fori_loop(0, E // (8 * FUSED), place_and_put, 0)
        lax.fori_loop(2 * E // (8 * FUSED), chunks, place, 0)

    @pl.when(inside < E)
    def _():
        lax.fori_loop(0, chunks, place, 0)
        off = lax.fori_loop(0, blocks_inside, put_eight, 0)
        off = lax.fori_loop(blocks_inside * 8, reach, put_both, off)
        lax.fori_loop(reach, E, put_far, off)

    zeros = jnp.zeros((GCH, GR, C), BF16)

    @pl.when(total <= KAG)
    def _():
        near_ref[pl.ds(total, GCH)] = zeros

    @pl.when(total > KAG)
    def _():
        spill[pl.ds(total - KAG + LEAD, GCH)] = zeros

    def send(k):
        return pltpu.make_async_copy(
            spill.at[pl.ds(LEAD + k * GCH, GCH)], far_hbm.at[pl.ds(k * GCH, GCH)], out_sem
        )

    def over(k, carry):
        send(k).start()
        send(k).wait()
        return carry

    lax.fori_loop(0, chunks - KA, over, 0)


def doubled(v, ids):
    top = jnp.broadcast_to(jnp.where(ids >= B // 2, 1.0, 0.0), (8, CH)).T
    mask = jnp.broadcast_to(top[:, 0:1], (CH, C)).astype(BF16)
    high = v * mask
    return v - high, high


def scalar(row):
    return jnp.min(row[:, 0:128].astype(F32)).astype(I32)


def window(ex_ref, k):
    return pl.multiple_of(lax.shift_right_logical(scalar(ex_ref[k]), 3) * 8, 8)


def margins_kernel(
    info_ref, w_ref, ids_ref, ex_ref, near_ref, far_hbm, out_ref, buf, acc, wide, tiles0, tiles1, sem
):
    chunks = lax.shift_right_logical(scalar(info_ref[1:2, :]) + (GCH - 1), 6)
    acc[...] = jnp.zeros_like(acc)
    wide[:, 0:C] = w_ref[0 : B // 2]
    wide[:, C : 2 * C] = w_ref[B // 2 : B]
    rows = iota((WIN, CH), 0)
    sub8 = iota((8, CH), 0)

    def prepare(k, tiles, source):
        low, high = doubled(source, ids_ref[k])
        tiles[:, 0:C] = low
        tiles[:, C : 2 * C] = high

    def multiply(tiles):
        return nt(wide[...], tiles[...])

    def choose(k, score, live):
        ids = ids_ref[k]
        ids8 = jnp.broadcast_to(ids, (8, CH))
        pieces = [score[8 * i : 8 * i + 8, :] for i in range(B // 16)]
        half = 8
        while len(pieces) > 1:
            bit = (ids8 & half) != 0
            pieces = [jnp.where(bit, b, a) for a, b in zip(pieces[0::2], pieces[1::2])]
            half *= 2
        pick = jnp.sum(jnp.where(sub8 == (ids8 & 7), pieces[0], 0.0), axis=0, keepdims=True)
        pick = jnp.where((ids >= 0) & live, pick, 0.0)
        base = window(ex_ref, k)
        span = pl.ds(base, WIN)
        acc[span, :] += jnp.where(rows + base == ex_ref[k], pick, 0.0)

    near = jnp.minimum(chunks, KA)
    final = near - 1

    def fetch(k):
        k = jnp.minimum(k, final)
        return k, near_ref[pl.ds(pl.multiple_of(k * CH, CH), CH), :]

    def ahead(k):
        for tiles, j in ((tiles0, k), (tiles1, k + 1)):
            j, v = fetch(j)
            prepare(j, tiles, v)

    ahead(0)

    def pair(i, carry):
        k = 2 * i
        choose(k, multiply(tiles0), k < near)
        choose(jnp.minimum(k + 1, final), multiply(tiles1), k + 1 < near)
        ahead(k + 2)
        return carry

    lax.fori_loop(0, lax.shift_right_logical(near + 1, 1), pair, 0)

    def outer(k, carry):
        copy = pltpu.make_async_copy(far_hbm.at[pl.ds(pl.multiple_of((k - KA) * CH, CH), CH)], buf, sem)
        copy.start()
        copy.wait()
        prepare(k, tiles0, buf[...])
        choose(k, multiply(tiles0), k < chunks)
        return carry

    lax.fori_loop(KA, chunks, outer, 0)
    row = jnp.sum(acc[0:E, :].T, axis=0, keepdims=True)
    out_ref[...] = jnp.broadcast_to(row[None], out_ref.shape)


def gradient_kernel(
    info_ref, parts_ref, ids_ref, ex_ref, near_ref, far_hbm, out_ref, buf, acc, column_ref,
    tiles0, tiles1, hot0, hot1, sem
):
    chunks = lax.shift_right_logical(scalar(info_ref[1:2, :]) + (GCH - 1), 6)
    acc[...] = jnp.zeros_like(acc)
    margin = jnp.sum(parts_ref[...].reshape(F, E), axis=0, keepdims=True)
    small_exp = jnp.exp(-jnp.abs(margin))
    label = info_ref[3:4, :].astype(F32)
    resid = jax.nn.sigmoid(margin) - label
    loss = jnp.sum(jnp.maximum(margin, 0.0) + jnp.log1p(small_exp) - label * margin)
    half = resid.astype(BF16).astype(F32)
    column_ref[0:E, :] = jnp.broadcast_to(half, (C, E)).T
    column_ref[E : E + WIN, :] = jnp.zeros((WIN, C), F32)
    rows = iota((WIN, CH), 0)
    lo_rows = iota((32, CH), 0)

    def prepare(k, tiles, hot, source, live):
        ids = ids_ref[k]
        base = window(ex_ref, k)
        column = column_ref[pl.ds(base, WIN), :]
        column = jnp.concatenate([column] * (CH // C), axis=1)
        coef = jnp.sum(jnp.where(rows + base == ex_ref[k], column, 0.0), axis=0, keepdims=True)
        coef = jnp.where((ids >= 0) & live, coef, 0.0)
        low = jnp.where(lo_rows == (ids & 31), coef, 0.0).astype(BF16)
        high = lax.shift_right_arithmetic(ids, 5) & 15
        hot[0:32, :] = low
        hot[32:48, :] = jnp.broadcast_to(high.astype(F32), (16, CH)).astype(BF16)
        lower, upper = doubled(source, ids)
        tiles[:, 0:C] = lower
        tiles[:, C : 2 * C] = upper

    def spread(hot):
        low = [hot[0:16, :], hot[16:32, :]]
        high = hot[32:48, :]
        zero = jnp.zeros((), BF16)
        return jnp.concatenate(
            [jnp.where(high == h, part, zero) for h in range(16) for part in low], axis=0
        )

    def multiply(tiles, hot):
        acc[...] += nn(spread(hot), tiles[...])

    near = jnp.minimum(chunks, KA)
    final = near - 1

    def fetch(k):
        live = k < near
        k = jnp.minimum(k, final)
        return k, near_ref[pl.ds(pl.multiple_of(k * CH, CH), CH), :], live

    def ahead(k):
        for tiles, hot, j in ((tiles0, hot0, k), (tiles1, hot1, k + 1)):
            j, v, live = fetch(j)
            prepare(j, tiles, hot, v, live)

    ahead(0)

    def pair(i, carry):
        acc[...] += nn(spread(hot0), tiles0[...]) + nn(spread(hot1), tiles1[...])
        ahead(2 * i + 2)
        return carry

    lax.fori_loop(0, lax.shift_right_logical(near + 1, 1), pair, 0)

    def outer(k, carry):
        copy = pltpu.make_async_copy(far_hbm.at[pl.ds(pl.multiple_of((k - KA) * CH, CH), CH)], buf, sem)
        copy.start()
        copy.wait()
        prepare(k, tiles0, hot0, buf[...], k < chunks)
        multiply(tiles0, hot0)
        return carry

    lax.fori_loop(KA, chunks, outer, 0)
    for i in range(2):
        out_ref[16 * i : 16 * i + 16, 0:32, :] = (
            acc[:, C * i : C * i + C].reshape(R // 2, 32, C).astype(BF16)
        )

    owner_hit = iota((R, E), 0) == info_ref[2:3, :]
    rank = info_ref[0:1, :]
    lane_row = iota((C, E), 0)
    extra = jnp.zeros((R, C), F32)
    for i, piece in enumerate(split3(margin)):
        a = jnp.where(owner_hit, piece, 0.0).astype(BF16)
        b = jnp.where(lane_row == rank + OWN * i, 1.0, 0.0).astype(BF16)
        extra = extra + nt(a, b)
    lane = iota((R, C), 1)
    for i, piece in enumerate(split3(jnp.full((R, C), loss, F32))):
        extra = jnp.where(lane == 3 * OWN + i, piece, extra)
    out_ref[:, 32 : 32 + XR, :] = jnp.broadcast_to(extra[:, None, :], (R, XR, C)).astype(BF16)


def finish_kernel(in_ref, grad_ref, owned_ref, loss_ref):
    total = in_ref[0, 0:32, :].astype(F32)
    for r in range(1, R):
        total = total + in_ref[r, 0:32, :].astype(F32)
    grad_ref[...] = total
    extra = in_ref[:, 32 : 32 + XR, :].astype(F32)[:, 0, :]
    src = iota((C, E), 0)
    pick = jnp.where((src < 3 * OWN) & ((src & 7) == (iota((C, E), 1) & 7)), 1.0, 0.0)
    wide = nn(extra.astype(BF16), pick.astype(BF16))
    own = lax.shift_right_logical(iota((R, E), 1), 3) == iota((R, E), 0)
    owned_ref[...] = jnp.sum(jnp.where(own, wide, 0.0), axis=0, keepdims=True)
    lane = iota((R, C), 1)
    keep = (lane >= 3 * OWN) & (lane < 3 * OWN + 3)
    total_loss = jnp.sum(jnp.where(keep, extra, 0.0), keepdims=True)
    loss_ref[...] = total_loss * (1.0 / (E * R))


def local(body, out_shapes, in_specs, out_specs, scratch, limit, *args):
    return pl.pallas_call(
        body,
        out_shape=out_shapes,
        in_specs=in_specs,
        out_specs=out_specs,
        scratch_shapes=scratch,
        compiler_params=pltpu.CompilerParams(vmem_limit_bytes=limit << 20),
    )(*args)


def near(x):
    return pltpu.with_memory_space_constraint(x, pltpu.VMEM)


def far(x):
    return pltpu.with_memory_space_constraint(x, pltpu.HBM)


def on_device(tile_values, tile_blocks, tile_counts, labels, owner_rank, weights):
    shape = jax.ShapeDtypeStruct
    dma = pltpu.SemaphoreType.DMA
    spread = local(
        spread_weights, pltpu.VMEM((R, B // R, C), BF16), [ANY], VMEM,
        [pltpu.VMEM((B // R, C), F32), dma(())], 4, far(weights),
    )
    table = lax.all_to_all(spread, "rows", 0, 0, tiled=True).reshape(B, C)
    owner_row = far(owner_rank.reshape(1, E))
    label_row = far(labels.reshape(1, E))
    packed, over, ids, ex, info = local(
        pack_tiles,
        (
            pltpu.VMEM((KAG + GCH, GR, C), BF16),
            pltpu.HBM((NG - KAG, GR, C), BF16),
            pltpu.VMEM((NCH, 1, CH), I32),
            pltpu.VMEM((NCH, 1, CH), I32),
            pltpu.VMEM((4, E), I32),
        ),
        [ANY, ANY, ANY, ANY, ANY, ANY],
        (VMEM, ANY, VMEM, VMEM, VMEM),
        [
            pltpu.SMEM((E,), I32),
            pltpu.VMEM((1, E), I32),
            pltpu.VMEM((SLOT, E), I32),
            pltpu.VMEM((1, E), I32),
            pltpu.VMEM((1, E), I32),
            pltpu.VMEM((NG, GR, C), BF16),
            pltpu.VMEM((NG - KAG + LEAD + GCH, GR, C), BF16),
            dma((5,)),
            dma((LOADS,)),
            dma(()),
        ],
        16,
        far(tile_counts.reshape(E)), far(tile_counts.T), far(tile_blocks.T), owner_row, label_row,
        far(tile_values.reshape(NG, GR, C)),
    )
    packed = packed.reshape(-1, C)
    over = over.reshape(-1, C)
    partial = local(
        margins_kernel, pltpu.VMEM((F, 1, E), F32), [VMEM, VMEM, VMEM, VMEM, VMEM, ANY], VMEM,
        [
            pltpu.VMEM((CH, C), BF16),
            pltpu.VMEM((E + WIN, CH), F32),
            pltpu.VMEM((B // 2, 2 * C), BF16),
            pltpu.VMEM((CH, 2 * C), BF16),
            pltpu.VMEM((CH, 2 * C), BF16),
            dma(()),
        ],
        16,
        near(info), near(table), near(ids), near(ex), near(packed), far(over),
    )
    parts = lax.all_to_all(partial, "feat", 0, 0, tiled=True)
    payload = local(
        gradient_kernel, pltpu.VMEM((R, B // R + XR, C), BF16),
        [VMEM, VMEM, VMEM, VMEM, VMEM, ANY], VMEM,
        [
            pltpu.VMEM((CH, C), BF16),
            pltpu.VMEM((B // 2, 2 * C), F32),
            pltpu.VMEM((E + WIN, C), F32),
            pltpu.VMEM((CH, 2 * C), BF16),
            pltpu.VMEM((CH, 2 * C), BF16),
            pltpu.VMEM((48, CH), BF16),
            pltpu.VMEM((48, CH), BF16),
            dma(()),
        ],
        16,
        near(info), near(parts), near(ids), near(ex), near(packed),
        far(over),
    )
    arrived = lax.all_to_all(payload, "rows", 0, 0, tiled=True)
    gradient, owned, loss = local(
        finish_kernel,
        (shape((B // R, C), F32), shape((1, E), F32), shape((1, 1), F32)),
        [VMEM], (VMEM, VMEM, VMEM), (), 8, near(arrived),
    )
    return owned.reshape(E), gradient, loss.reshape(())


def solution(mesh):
    in_specs = (
        P("rows", "feat", None),
        P("rows", "feat"),
        P("rows", "feat"),
        P("rows"),
        P("rows"),
        P(("feat", "rows"), None),
    )
    out_specs = (P("rows"), P(("feat", "rows"), None), P())
    return jax.shard_map(
        on_device, mesh=mesh, in_specs=in_specs, out_specs=out_specs, check_vma=False
    )
```

```python
import jax
import jax.numpy as jnp
from jax import lax
from jax.experimental import pallas as pl
from jax.experimental.pallas import tpu as pltpu
from jax.sharding import PartitionSpec as P

F32 = jnp.float32
BF16 = jnp.bfloat16
I32 = jnp.int32

E = 256
SLOT = 64
C = 128
B = 1024
R = 32
F = 8
OWN = 8
GR = 8
NG = E * SLOT // GR
CH = 512
GCH = CH // GR
NCH = NG // GCH
KA = 10
KF = NCH - KA
XR = 8
WIN = GCH + 8
FUSED = 4
EARLY = 2
LOADS = 4

VMEM = pl.BlockSpec(memory_space=pltpu.VMEM)
ANY = pl.BlockSpec(memory_space=pl.ANY)


def nt(a, b):
    return lax.dot_general(a, b, (((1,), (1,)), ((), ())), preferred_element_type=F32)


def nn(a, b):
    return lax.dot_general(a, b, (((1,), (0,)), ((), ())), preferred_element_type=F32)


def split3(x):
    hi = x.astype(BF16).astype(F32)
    mid = (x - hi).astype(BF16).astype(F32)
    lo = (x - hi - mid).astype(BF16).astype(F32)
    return hi, mid, lo


def iota(shape, dim):
    return lax.broadcasted_iota(I32, shape, dim)


def spread_weights(w_hbm, out_ref, w_ref, sem):
    pltpu.make_async_copy(w_hbm, w_ref, sem).start()
    pltpu.make_async_copy(w_hbm, w_ref, sem).wait()
    half = w_ref[...].astype(BF16)
    both = jnp.concatenate([half[0:16], half[16:32]], axis=1)
    out_ref[...] = jnp.broadcast_to(both[None], out_ref.shape)


def pack_tiles(
    flat_hbm, counts_hbm, blocks_hbm, owner_hbm, labels_hbm, values_hbm, near_ref, far_hbm, ids_ref,
    ex_ref, info_ref, counts_s, counts_ref, blocks_ref, owner_ref, labels_ref, values, packed, spill,
    small_sems, sems, out_sem
):
    part = NG // LOADS
    small = [
        pltpu.make_async_copy(src, dst, small_sems.at[i])
        for i, (src, dst) in enumerate(
            [
                (counts_hbm, counts_ref),
                (blocks_hbm, blocks_ref),
                (owner_hbm, owner_ref),
                (flat_hbm, counts_s),
                (labels_hbm, labels_ref),
            ]
        )
    ]
    loads = [
        pltpu.make_async_copy(
            values_hbm.at[pl.ds(i * part, part)], values.at[pl.ds(i * part, part)], sems.at[i]
        )
        for i in range(LOADS)
    ]
    for copy in small + loads:
        copy.start()
    for copy in small:
        copy.wait()

    counts = counts_ref[...]
    granules = lax.shift_right_logical(counts + (GR - 1), 3).astype(F32)
    spread = jnp.broadcast_to(granules, (E, E)).astype(BF16)
    up = iota((E, E), 0)
    across = iota((E, E), 1)
    first = nt((across < up).astype(F32).astype(BF16), spread)
    first = jnp.concatenate([first] * (CH // E), axis=1)
    before = (up < across).astype(F32).astype(BF16)
    start = nn(spread[0:16], before)
    start_hi = jnp.floor(start * (1.0 / 64.0))
    start_lo = start - 64.0 * start_hi
    row16 = iota((16, E), 0)
    tail = jnp.where(row16 == 0, start_hi, jnp.where(row16 == 1, start_lo, iota((16, E), 1).astype(F32)))
    ids = jnp.where(iota((SLOT, E), 0) < counts, blocks_ref[...], 2047)
    both = jnp.concatenate([lax.shift_right_logical(ids, 5), ids & 31], axis=0).astype(F32)
    table = jnp.concatenate([both, tail], axis=0)
    shifted = jnp.where(iota(table.shape, 1) == 0, 0.0, pltpu.roll(table, 1, 1))
    table = (table - shifted).astype(BF16)
    lane = iota((1, CH), 1)
    sub = iota((SLOT, CH), 0).astype(F32)
    total = jnp.sum(granules).astype(I32)
    chunks = lax.shift_right_logical(total + (GCH - 1), 6)

    hits = (iota((R, E), 0) == owner_ref[...]).astype(F32)
    earlier = nn(hits.astype(BF16), before)
    info_ref[0:1, :] = jnp.sum(hits * earlier, axis=0, keepdims=True).astype(I32)
    info_ref[1:2, :] = jnp.full((1, E), total, I32)
    info_ref[2:3, :] = owner_ref[...]
    info_ref[3:4, :] = labels_ref[...]

    def place(k, carry):
        pos = k * CH + lane
        gran = lax.shift_right_logical(pos, 3).astype(F32)
        x = nn(table, jnp.where(first <= gran, 1.0, 0.0).astype(BF16))
        slot = pos.astype(F32) - 8.0 * (64.0 * x[128:129] + x[129:130])
        code = 32.0 * x[0:64] + x[64:128]
        here = jnp.sum(jnp.where(sub == slot, code, 0.0), axis=0, keepdims=True).astype(I32)
        live = (pos < total * GR) & (here < B)
        ids_ref[k] = jnp.where(live, here, -1)
        ex_ref[k] = x[130:131].astype(I32)
        return carry


    def put_eight(i, off):
        for j in range(8):
            e = i * 8 + j
            packed[pl.ds(off, 8)] = values[pl.ds(e * 8, 8)]
            off = off + lax.shift_right_logical(counts_s[e] + (GR - 1), 3)
        return off

    def place_two(i, carry):
        place(2 * i, 0)
        return place(2 * i + 1, carry)

    def place_and_put(i, off):
        place(EARLY + i, 0)
        for j in range(FUSED):
            off = put_eight(FUSED * i + j, off)
        return off

    lax.fori_loop(0, EARLY // 2, place_two, 0)
    for copy in loads:
        copy.wait()
    lax.fori_loop(0, E // (8 * FUSED), place_and_put, 0)
    lax.fori_loop(EARLY + E // (8 * FUSED), chunks, place, 0)
    packed[pl.ds(total, GCH)] = jnp.zeros((GCH, GR, C), BF16)

    def widen(k, out, at):
        low, high = doubled(packed[pl.ds(k * GCH, GCH)].reshape(CH, C), ids_ref[k])
        span = pl.ds(pl.multiple_of(at * CH, CH), CH)
        out[span, 0:C] = low
        out[span, C : 2 * C] = high

    near = jnp.minimum(chunks, KA)

    def widen_pair(i, carry):
        for k in (2 * i, jnp.minimum(2 * i + 1, near - 1)):
            widen(k, near_ref, k)
        return carry

    lax.fori_loop(0, lax.shift_right_logical(near + 1, 1), widen_pair, 0)

    def send(k):
        span = pl.ds(pl.multiple_of(k * CH, CH), CH)
        return pltpu.make_async_copy(spill.at[span], far_hbm.at[span], out_sem.at[k])

    def over(k, carry):
        widen(k + KA, spill, k)
        send(k).start()
        return carry

    def arrive(k, carry):
        send(k).wait()
        return carry

    lax.fori_loop(0, chunks - KA, over, 0)
    lax.fori_loop(0, chunks - KA, arrive, 0)


def doubled(v, ids):
    top = jnp.broadcast_to(jnp.where((ids & 16) != 0, 1.0, 0.0), (8, CH)).T
    mask = jnp.broadcast_to(top[:, 0:1], (CH, C)).astype(BF16)
    high = v * mask
    return v - high, high


def scalar(row):
    return jnp.min(row[:, 0:128].astype(F32)).astype(I32)


def window(ex_ref, k):
    return pl.multiple_of(lax.shift_right_logical(scalar(ex_ref[k]), 3) * 8, 8)


def each_chunk(info_ref, near_ref, far_hbm, buf, sems, pair, single):
    chunks = lax.shift_right_logical(scalar(info_ref[1:2, :]) + (GCH - 1), 6)
    near = jnp.minimum(chunks, KA)

    def fetch(k):
        span = pl.ds(pl.multiple_of(k * CH, CH), CH)
        return pltpu.make_async_copy(far_hbm.at[span], buf.at[span], sems.at[k])

    def start(k, carry):
        fetch(k).start()
        return carry

    lax.fori_loop(0, chunks - KA, start, 0)

    def tiles(ref, k):
        return ref[pl.ds(pl.multiple_of(k * CH, CH), CH), :]

    def inner(i, carry):
        k0 = 2 * i
        k1 = jnp.minimum(k0 + 1, near - 1)
        pair(k0, tiles(near_ref, k0), k1, tiles(near_ref, k1), k0 + 1 < near)
        return carry

    lax.fori_loop(0, lax.shift_right_logical(near + 1, 1), inner, 0)

    def outer(k, carry):
        fetch(k).wait()
        single(k + KA, tiles(buf, k))
        return carry

    lax.fori_loop(0, chunks - KA, outer, 0)


def margins_kernel(
    info_ref, w_ref, ids_ref, ex_ref, near_ref, far_hbm, out_ref, buf, acc, sems
):
    acc[...] = jnp.zeros_like(acc)
    rows = iota((WIN, CH), 0)
    sub8 = iota((8, CH), 0)

    def choose(k, score, live):
        ids = ids_ref[k]
        ids8 = jnp.broadcast_to(ids, (8, CH))
        pieces = [score[8 * i : 8 * i + 8, :] for i in range(B // 16)]
        half = 8
        while len(pieces) > 1:
            bit = (ids8 & half) != 0
            pieces = [jnp.where(bit, b, a) for a, b in zip(pieces[0::2], pieces[1::2])]
            half = 32 if half == 8 else 2 * half
        pick = jnp.sum(jnp.where(sub8 == (ids8 & 7), pieces[0], 0.0), axis=0, keepdims=True)
        pick = jnp.where((ids >= 0) & live, pick, 0.0)
        base = window(ex_ref, k)
        span = pl.ds(base, WIN)
        acc[span, :] += jnp.where(rows + base == ex_ref[k], pick, 0.0)

    def single(k, v):
        choose(k, nt(w_ref[...], v), True)

    def pair(k0, v0, k1, v1, live):
        choose(k0, nt(w_ref[...], v0), True)
        choose(k1, nt(w_ref[...], v1), live)

    each_chunk(info_ref, near_ref, far_hbm, buf, sems, pair, single)
    folded = acc[0:E, 0:C]
    for i in range(1, CH // C):
        folded = folded + acc[0:E, C * i : C * i + C]
    row = jnp.sum(folded.T, axis=0, keepdims=True)
    out_ref[...] = jnp.broadcast_to(row[None], out_ref.shape)


def gradient_kernel(
    info_ref, parts_ref, ids_ref, ex_ref, near_ref, far_hbm, out_ref, buf, acc, column_ref, hot0, hot1,
    sems
):
    acc[...] = jnp.zeros_like(acc)
    margin = jnp.sum(parts_ref[...].reshape(F, E), axis=0, keepdims=True)
    small_exp = jnp.exp(-jnp.abs(margin))
    label = info_ref[3:4, :].astype(F32)
    resid = jax.nn.sigmoid(margin) - label
    loss = jnp.sum(jnp.maximum(margin, 0.0) + jnp.log1p(small_exp) - label * margin)
    half = resid.astype(BF16).astype(F32)
    column_ref[0:E, :] = jnp.broadcast_to(half, (C, E)).T
    column_ref[E : E + WIN, :] = jnp.zeros((WIN, C), F32)
    rows = iota((WIN, CH), 0)
    lo_rows = iota((16, CH), 0)

    def prepare(k, hot, live):
        ids = ids_ref[k]
        base = window(ex_ref, k)
        column = column_ref[pl.ds(base, WIN), :]
        column = jnp.concatenate([column] * (CH // C), axis=1)
        coef = jnp.sum(jnp.where(rows + base == ex_ref[k], column, 0.0), axis=0, keepdims=True)
        coef = jnp.where((ids >= 0) & live, coef, 0.0)
        hot[0:16, :] = jnp.where(lo_rows == (ids & 15), coef, 0.0).astype(BF16)
        high = lax.shift_right_arithmetic(ids, 5).astype(F32)
        hot[16:32, :] = jnp.broadcast_to(high, (16, CH)).astype(BF16)

    def spread(hot):
        low = hot[0:16, :]
        high = hot[16:32, :]
        zero = jnp.zeros((), BF16)
        return jnp.concatenate([jnp.where(high == h, low, zero) for h in range(32)], axis=0)

    def single(k, v):
        prepare(k, hot0, True)
        acc[...] += nn(spread(hot0), v)

    chunks = lax.shift_right_logical(scalar(info_ref[1:2, :]) + (GCH - 1), 6)
    near = jnp.minimum(chunks, KA)

    def ahead(k):
        for hot, j in ((hot0, k), (hot1, k + 1)):
            prepare(jnp.minimum(j, near - 1), hot, j < near)

    ahead(0)

    def pair(k0, v0, k1, v1, live):
        acc[...] += nn(spread(hot0), v0) + nn(spread(hot1), v1)
        ahead(k0 + 2)

    each_chunk(info_ref, near_ref, far_hbm, buf, sems, pair, single)
    for i in range(2):
        out_ref[:, 16 * i : 16 * i + 16, :] = (
            acc[:, C * i : C * i + C].reshape(R, 16, C).astype(BF16)
        )

    owner_hit = iota((R, E), 0) == info_ref[2:3, :]
    rank = info_ref[0:1, :]
    lane_row = iota((C, E), 0)
    extra = jnp.zeros((R, C), F32)
    for i, piece in enumerate(split3(margin)):
        a = jnp.where(owner_hit, piece, 0.0).astype(BF16)
        b = jnp.where(lane_row == rank + OWN * i, 1.0, 0.0).astype(BF16)
        extra = extra + nt(a, b)
    lane = iota((R, C), 1)
    for i, piece in enumerate(split3(jnp.full((R, C), loss, F32))):
        extra = jnp.where(lane == 3 * OWN + i, piece, extra)
    out_ref[:, 32 : 32 + XR, :] = jnp.broadcast_to(extra[:, None, :], (R, XR, C)).astype(BF16)


def finish_kernel(in_ref, grad_ref, owned_ref, loss_ref):
    total = in_ref[0, 0:32, :].astype(F32)
    for r in range(1, R):
        total = total + in_ref[r, 0:32, :].astype(F32)
    grad_ref[...] = total
    extra = in_ref[:, 32 : 32 + XR, :].astype(F32)[:, 0, :]
    src = iota((C, E), 0)
    pick = jnp.where((src < 3 * OWN) & ((src & 7) == (iota((C, E), 1) & 7)), 1.0, 0.0)
    wide = nn(extra.astype(BF16), pick.astype(BF16))
    own = lax.shift_right_logical(iota((R, E), 1), 3) == iota((R, E), 0)
    owned_ref[...] = jnp.sum(jnp.where(own, wide, 0.0), axis=0, keepdims=True)
    lane = iota((R, C), 1)
    keep = (lane >= 3 * OWN) & (lane < 3 * OWN + 3)
    total_loss = jnp.sum(jnp.where(keep, extra, 0.0), keepdims=True)
    loss_ref[...] = total_loss * (1.0 / (E * R))


def local(body, out_shapes, in_specs, out_specs, scratch, limit, *args):
    return pl.pallas_call(
        body,
        out_shape=out_shapes,
        in_specs=in_specs,
        out_specs=out_specs,
        scratch_shapes=scratch,
        compiler_params=pltpu.CompilerParams(vmem_limit_bytes=limit << 20),
    )(*args)


def near(x):
    return pltpu.with_memory_space_constraint(x, pltpu.VMEM)


def far(x):
    return pltpu.with_memory_space_constraint(x, pltpu.HBM)


def on_device(tile_values, tile_blocks, tile_counts, labels, owner_rank, weights):
    shape = jax.ShapeDtypeStruct
    dma = pltpu.SemaphoreType.DMA
    spread = local(
        spread_weights, pltpu.VMEM((R, B // (2 * R), 2 * C), BF16), [ANY], VMEM,
        [pltpu.VMEM((B // R, C), F32), dma(())], 4, far(weights),
    )
    table = lax.all_to_all(spread, "rows", 0, 0, tiled=True).reshape(B // 2, 2 * C)
    owner_row = far(owner_rank.reshape(1, E))
    label_row = far(labels.reshape(1, E))
    packed, over, ids, ex, info = local(
        pack_tiles,
        (
            pltpu.VMEM((KA * CH, 2 * C), BF16),
            pltpu.HBM((KF * CH, 2 * C), BF16),
            pltpu.VMEM((NCH, 1, CH), I32),
            pltpu.VMEM((NCH, 1, CH), I32),
            pltpu.VMEM((4, E), I32),
        ),
        [ANY, ANY, ANY, ANY, ANY, ANY],
        (VMEM, ANY, VMEM, VMEM, VMEM),
        [
            pltpu.SMEM((E,), I32),
            pltpu.VMEM((1, E), I32),
            pltpu.VMEM((SLOT, E), I32),
            pltpu.VMEM((1, E), I32),
            pltpu.VMEM((1, E), I32),
            pltpu.VMEM((NG, GR, C), BF16),
            pltpu.VMEM((NG + GCH, GR, C), BF16),
            pltpu.VMEM((KF * CH, 2 * C), BF16),
            dma((5,)),
            dma((LOADS,)),
            dma((KF,)),
        ],
        24,
        far(tile_counts.reshape(E)), far(tile_counts.T), far(tile_blocks.T), owner_row, label_row,
        far(tile_values.reshape(NG, GR, C)),
    )
    partial = local(
        margins_kernel, pltpu.VMEM((F, 1, E), F32), [VMEM, VMEM, VMEM, VMEM, VMEM, ANY], VMEM,
        [
            pltpu.VMEM((KF * CH, 2 * C), BF16),
            pltpu.VMEM((E + WIN, CH), F32),
            dma((KF,)),
        ],
        16,
        near(info), near(table), near(ids), near(ex), near(packed), far(over),
    )
    parts = lax.all_to_all(partial, "feat", 0, 0, tiled=True)
    payload = local(
        gradient_kernel, pltpu.VMEM((R, B // R + XR, C), BF16),
        [VMEM, VMEM, VMEM, VMEM, VMEM, ANY], VMEM,
        [
            pltpu.VMEM((KF * CH, 2 * C), BF16),
            pltpu.VMEM((B // 2, 2 * C), F32),
            pltpu.VMEM((E + WIN, C), F32),
            pltpu.VMEM((32, CH), BF16),
            pltpu.VMEM((32, CH), BF16),
            dma((KF,)),
        ],
        16,
        near(info), near(parts), near(ids), near(ex), near(packed),
        far(over),
    )
    arrived = lax.all_to_all(payload, "rows", 0, 0, tiled=True)
    gradient, owned, loss = local(
        finish_kernel,
        (shape((B // R, C), F32), shape((1, E), F32), shape((1, 1), F32)),
        [VMEM], (VMEM, VMEM, VMEM), (), 8, near(arrived),
    )
    return owned.reshape(E), gradient, loss.reshape(())


def solution(mesh):
    in_specs = (
        P("rows", "feat", None),
        P("rows", "feat"),
        P("rows", "feat"),
        P("rows"),
        P("rows"),
        P(("feat", "rows"), None),
    )
    out_specs = (P("rows"), P(("feat", "rows"), None), P())
    return jax.shard_map(
        on_device, mesh=mesh, in_specs=in_specs, out_specs=out_specs, check_vma=False
    )
```

```python
import jax
import jax.numpy as jnp
from jax import lax
from jax.experimental import pallas as pl
from jax.experimental.pallas import tpu as pltpu
from jax.sharding import PartitionSpec as P

F32 = jnp.float32
BF16 = jnp.bfloat16
I32 = jnp.int32

E = 256
SLOT = 64
C = 128
B = 1024
R = 32
F = 8
OWN = 8
GR = 8
NG = E * SLOT // GR
CH = 512
GCH = CH // GR
NCH = NG // GCH
KA = 11
KF = NCH - KA
GROUP = 11
XR = 8
WIN = GCH + 8
FUSED = 4
EARLY = 2
LOADS = 4

VMEM = pl.BlockSpec(memory_space=pltpu.VMEM)
ANY = pl.BlockSpec(memory_space=pl.ANY)


def nt(a, b):
    return lax.dot_general(a, b, (((1,), (1,)), ((), ())), preferred_element_type=F32)


def nn(a, b):
    return lax.dot_general(a, b, (((1,), (0,)), ((), ())), preferred_element_type=F32)


def split3(x):
    hi = x.astype(BF16).astype(F32)
    mid = (x - hi).astype(BF16).astype(F32)
    lo = (x - hi - mid).astype(BF16).astype(F32)
    return hi, mid, lo


def iota(shape, dim):
    return lax.broadcasted_iota(I32, shape, dim)


def spread_weights(w_hbm, out_ref, w_ref, sem):
    pltpu.make_async_copy(w_hbm, w_ref, sem).start()
    pltpu.make_async_copy(w_hbm, w_ref, sem).wait()
    half = w_ref[...].astype(BF16)
    both = jnp.concatenate([half[0:16], half[16:32]], axis=1)
    out_ref[...] = jnp.broadcast_to(both[None], out_ref.shape)


def pack_tiles(
    flat_hbm, counts_hbm, blocks_hbm, owner_hbm, labels_hbm, values_hbm, near_ref, far_hbm, ids_ref,
    ex_ref, info_ref, counts_s, counts_ref, blocks_ref, owner_ref, labels_ref, values, packed, spill,
    small_sems, sems, out_sem
):
    part = NG // LOADS
    small = [
        pltpu.make_async_copy(src, dst, small_sems.at[i])
        for i, (src, dst) in enumerate(
            [
                (counts_hbm, counts_ref),
                (blocks_hbm, blocks_ref),
                (owner_hbm, owner_ref),
                (flat_hbm, counts_s),
                (labels_hbm, labels_ref),
            ]
        )
    ]
    loads = [
        pltpu.make_async_copy(
            values_hbm.at[pl.ds(i * part, part)], values.at[pl.ds(i * part, part)], sems.at[i]
        )
        for i in range(LOADS)
    ]
    for copy in small + loads:
        copy.start()
    for copy in small:
        copy.wait()

    counts = counts_ref[...]
    granules = lax.shift_right_logical(counts + (GR - 1), 3).astype(F32)
    spread = jnp.broadcast_to(granules, (E, E)).astype(BF16)
    up = iota((E, E), 0)
    across = iota((E, E), 1)
    first = nt((across < up).astype(F32).astype(BF16), spread)
    first = jnp.concatenate([first] * (CH // E), axis=1)
    before = (up < across).astype(F32).astype(BF16)
    start = nn(spread[0:16], before)
    start_hi = jnp.floor(start * (1.0 / 64.0))
    start_lo = start - 64.0 * start_hi
    row16 = iota((16, E), 0)
    tail = jnp.where(row16 == 0, start_hi, jnp.where(row16 == 1, start_lo, iota((16, E), 1).astype(F32)))
    ids = jnp.where(iota((SLOT, E), 0) < counts, blocks_ref[...], 2047)
    both = jnp.concatenate([lax.shift_right_logical(ids, 5), ids & 31], axis=0).astype(F32)
    table = jnp.concatenate([both, tail], axis=0)
    shifted = jnp.where(iota(table.shape, 1) == 0, 0.0, pltpu.roll(table, 1, 1))
    table = (table - shifted).astype(BF16)
    lane = iota((1, CH), 1)
    sub = iota((SLOT, CH), 0).astype(F32)
    total = jnp.sum(granules).astype(I32)
    chunks = lax.shift_right_logical(total + (GCH - 1), 6)

    hits = (iota((R, E), 0) == owner_ref[...]).astype(F32)
    earlier = nn(hits.astype(BF16), before)
    info_ref[0:1, :] = jnp.sum(hits * earlier, axis=0, keepdims=True).astype(I32)
    info_ref[1:2, :] = jnp.full((1, E), total, I32)
    info_ref[2:3, :] = owner_ref[...]
    info_ref[3:4, :] = labels_ref[...]

    def place(k, carry):
        pos = k * CH + lane
        gran = lax.shift_right_logical(pos, 3).astype(F32)
        x = nn(table, jnp.where(first <= gran, 1.0, 0.0).astype(BF16))
        slot = pos.astype(F32) - 8.0 * (64.0 * x[128:129] + x[129:130])
        code = 32.0 * x[0:64] + x[64:128]
        here = jnp.sum(jnp.where(sub == slot, code, 0.0), axis=0, keepdims=True).astype(I32)
        live = (pos < total * GR) & (here < B)
        ids_ref[k] = jnp.where(live, here, -1)
        ex_ref[k] = x[130:131].astype(I32)
        return carry


    def put_eight(i, off):
        for j in range(8):
            e = i * 8 + j
            packed[pl.ds(off, 8)] = values[pl.ds(e * 8, 8)]
            off = off + lax.shift_right_logical(counts_s[e] + (GR - 1), 3)
        return off

    def place_two(i, carry):
        place(2 * i, 0)
        return place(2 * i + 1, carry)

    def place_and_put(i, off):
        place(EARLY + i, 0)
        for j in range(FUSED):
            off = put_eight(FUSED * i + j, off)
        return off

    lax.fori_loop(0, EARLY // 2, place_two, 0)
    for copy in loads:
        copy.wait()
    lax.fori_loop(0, E // (8 * FUSED), place_and_put, 0)
    lax.fori_loop(EARLY + E // (8 * FUSED), chunks, place, 0)
    packed[pl.ds(total, GCH)] = jnp.zeros((GCH, GR, C), BF16)

    def widen(k, out, at):
        low, high = doubled(packed[pl.ds(k * GCH, GCH)].reshape(CH, C), ids_ref[k])
        span = pl.ds(pl.multiple_of(at * CH, CH), CH)
        out[span, 0:C] = low
        out[span, C : 2 * C] = high

    near = jnp.minimum(chunks, KA)

    def widen_pair(i, carry):
        for k in (2 * i, 2 * i + 1):
            k = jnp.minimum(k, full - 1)
            widen(jnp.minimum(k, near - 1), near_ref, k)
        return carry

    full = groups(near) * GROUP
    lax.fori_loop(0, lax.shift_right_logical(full + 1, 1), widen_pair, 0)

    def send(k):
        span = pl.ds(pl.multiple_of(k * CH, CH), CH)
        return pltpu.make_async_copy(spill.at[span], far_hbm.at[span], out_sem.at[k])

    def over(k, carry):
        widen(k + KA, spill, k)
        send(k).start()
        return carry

    def arrive(k, carry):
        send(k).wait()
        return carry

    lax.fori_loop(0, chunks - KA, over, 0)
    lax.fori_loop(0, chunks - KA, arrive, 0)


def groups(near):
    return lax.div(near + (GROUP - 1), GROUP)


def doubled(v, ids):
    top = jnp.broadcast_to(jnp.where((ids & 16) != 0, 1.0, 0.0), (8, CH)).T
    mask = jnp.broadcast_to(top[:, 0:1], (CH, C)).astype(BF16)
    high = v * mask
    return v - high, high


def scalar(row):
    return jnp.min(row[:, 0:128].astype(F32)).astype(I32)


def window(ex_ref, k):
    return pl.multiple_of(lax.shift_right_logical(scalar(ex_ref[k]), 3) * 8, 8)


def tiles(ref, k, n):
    return ref[pl.ds(pl.multiple_of(k * CH, CH), n * CH), :]


def each_chunk(info_ref, far_hbm, buf, sems, group, single):
    chunks = lax.shift_right_logical(scalar(info_ref[1:2, :]) + (GCH - 1), 6)
    near = jnp.minimum(chunks, KA)

    def fetch(k):
        span = pl.ds(pl.multiple_of(k * CH, CH), CH)
        return pltpu.make_async_copy(far_hbm.at[span], buf.at[span], sems.at[k])

    def start(k, carry):
        fetch(k).start()
        return carry

    lax.fori_loop(0, chunks - KA, start, 0)

    def inner(i, carry):
        group(i * GROUP, near)
        return carry

    lax.fori_loop(0, groups(near), inner, 0)

    def outer(k, carry):
        fetch(k).wait()
        single(k + KA, tiles(buf, k, 1))
        return carry

    lax.fori_loop(0, chunks - KA, outer, 0)


def margins_kernel(
    info_ref, w_ref, ids_ref, ex_ref, near_ref, far_hbm, out_ref, buf, acc, sems
):
    acc[...] = jnp.zeros_like(acc)
    rows = iota((WIN, CH), 0)
    sub8 = iota((8, CH), 0)

    def choose(k, score, live):
        ids = ids_ref[k]
        ids8 = jnp.broadcast_to(ids, (8, CH))
        pieces = [score[8 * i : 8 * i + 8, :] for i in range(B // 16)]
        half = 8
        while len(pieces) > 1:
            bit = (ids8 & half) != 0
            pieces = [jnp.where(bit, b, a) for a, b in zip(pieces[0::2], pieces[1::2])]
            half = 32 if half == 8 else 2 * half
        pick = jnp.sum(jnp.where(sub8 == (ids8 & 7), pieces[0], 0.0), axis=0, keepdims=True)
        pick = jnp.where((ids >= 0) & live, pick, 0.0)
        base = window(ex_ref, k)
        span = pl.ds(base, WIN)
        acc[span, :] += jnp.where(rows + base == ex_ref[k], pick, 0.0)

    def single(k, v):
        choose(k, nt(w_ref[...], v), True)

    def group(k, near):
        for j in range(GROUP):
            choose(jnp.minimum(k + j, near - 1), nt(w_ref[...], tiles(near_ref, k + j, 1)), k + j < near)

    each_chunk(info_ref, far_hbm, buf, sems, group, single)
    folded = acc[0:E, 0:C]
    for i in range(1, CH // C):
        folded = folded + acc[0:E, C * i : C * i + C]
    row = jnp.sum(folded.T, axis=0, keepdims=True)
    out_ref[...] = jnp.broadcast_to(row[None], out_ref.shape)


def gradient_kernel(
    info_ref, parts_ref, ids_ref, ex_ref, near_ref, far_hbm, out_ref, buf, acc, column_ref, hots, sems
):
    acc[...] = jnp.zeros_like(acc)
    margin = jnp.sum(parts_ref[...].reshape(F, E), axis=0, keepdims=True)
    small_exp = jnp.exp(-jnp.abs(margin))
    label = info_ref[3:4, :].astype(F32)
    resid = jax.nn.sigmoid(margin) - label
    loss = jnp.sum(jnp.maximum(margin, 0.0) + jnp.log1p(small_exp) - label * margin)
    half = resid.astype(BF16).astype(F32)
    column_ref[0:E, :] = jnp.broadcast_to(half, (C, E)).T
    column_ref[E : E + WIN, :] = jnp.zeros((WIN, C), F32)

    owner_hit = iota((R, E), 0) == info_ref[2:3, :]
    rank = info_ref[0:1, :]
    lane_row = iota((C, E), 0)
    extra = jnp.zeros((R, C), F32)
    for i, piece in enumerate(split3(margin)):
        a = jnp.where(owner_hit, piece, 0.0).astype(BF16)
        b = jnp.where(lane_row == rank + OWN * i, 1.0, 0.0).astype(BF16)
        extra = extra + nt(a, b)
    lane = iota((R, C), 1)
    for i, piece in enumerate(split3(jnp.full((R, C), loss, F32))):
        extra = jnp.where(lane == 3 * OWN + i, piece, extra)
    out_ref[:, 32 : 32 + XR, :] = jnp.broadcast_to(extra[:, None, :], (R, XR, C)).astype(BF16)

    rows = iota((WIN, CH), 0)
    lo_rows = iota((16, CH), 0)

    def prepare(k, j, live):
        hot = hots.at[j]
        ids = ids_ref[k]
        base = window(ex_ref, k)
        column = column_ref[pl.ds(base, WIN), :]
        column = jnp.concatenate([column] * (CH // C), axis=1)
        coef = jnp.sum(jnp.where(rows + base == ex_ref[k], column, 0.0), axis=0, keepdims=True)
        coef = jnp.where((ids >= 0) & live, coef, 0.0)
        hot[0:16, :] = jnp.where(lo_rows == (ids & 15), coef, 0.0).astype(BF16)
        high = lax.shift_right_arithmetic(ids, 5).astype(F32)
        hot[16:32, :] = jnp.broadcast_to(high, (16, CH)).astype(BF16)

    def spread(j):
        low = hots[j, 0:16, :]
        high = hots[j, 16:32, :]
        zero = jnp.zeros((), BF16)
        return jnp.concatenate([jnp.where(high == h, low, zero) for h in range(32)], axis=0)

    def single(k, v):
        prepare(k, 0, True)
        acc[...] += nn(spread(0), v)

    chunks = lax.shift_right_logical(scalar(info_ref[1:2, :]) + (GCH - 1), 6)
    near = jnp.minimum(chunks, KA)

    def ahead(k):
        for j in range(GROUP):
            prepare(jnp.minimum(k + j, near - 1), j, k + j < near)

    ahead(0)

    def group(k, near):
        hot = jnp.concatenate([spread(j) for j in range(GROUP)], axis=1)
        acc[...] += nn(hot, tiles(near_ref, k, GROUP))
        ahead(k + GROUP)

    each_chunk(info_ref, far_hbm, buf, sems, group, single)
    for i in range(2):
        out_ref[:, 16 * i : 16 * i + 16, :] = (
            acc[:, C * i : C * i + C].reshape(R, 16, C).astype(BF16)
        )


def finish_kernel(in_ref, grad_ref, owned_ref, loss_ref):
    total = in_ref[0, 0:32, :].astype(F32)
    for r in range(1, R):
        total = total + in_ref[r, 0:32, :].astype(F32)
    grad_ref[...] = total
    extra = in_ref[:, 32 : 32 + XR, :].astype(F32)[:, 0, :]
    src = iota((C, E), 0)
    pick = jnp.where((src < 3 * OWN) & ((src & 7) == (iota((C, E), 1) & 7)), 1.0, 0.0)
    wide = nn(extra.astype(BF16), pick.astype(BF16))
    own = lax.shift_right_logical(iota((R, E), 1), 3) == iota((R, E), 0)
    owned_ref[...] = jnp.sum(jnp.where(own, wide, 0.0), axis=0, keepdims=True)
    lane = iota((R, C), 1)
    keep = (lane >= 3 * OWN) & (lane < 3 * OWN + 3)
    total_loss = jnp.sum(jnp.where(keep, extra, 0.0), keepdims=True)
    loss_ref[...] = total_loss * (1.0 / (E * R))


def local(body, out_shapes, in_specs, out_specs, scratch, limit, *args):
    return pl.pallas_call(
        body,
        out_shape=out_shapes,
        in_specs=in_specs,
        out_specs=out_specs,
        scratch_shapes=scratch,
        compiler_params=pltpu.CompilerParams(vmem_limit_bytes=limit << 20),
    )(*args)


def near(x):
    return pltpu.with_memory_space_constraint(x, pltpu.VMEM)


def far(x):
    return pltpu.with_memory_space_constraint(x, pltpu.HBM)


def on_device(tile_values, tile_blocks, tile_counts, labels, owner_rank, weights):
    shape = jax.ShapeDtypeStruct
    dma = pltpu.SemaphoreType.DMA
    spread = local(
        spread_weights, pltpu.VMEM((R, B // (2 * R), 2 * C), BF16), [ANY], VMEM,
        [pltpu.VMEM((B // R, C), F32), dma(())], 4, far(weights),
    )
    table = lax.all_to_all(spread, "rows", 0, 0, tiled=True).reshape(B // 2, 2 * C)
    owner_row = far(owner_rank.reshape(1, E))
    label_row = far(labels.reshape(1, E))
    packed, over, ids, ex, info = local(
        pack_tiles,
        (
            pltpu.VMEM((KA * CH, 2 * C), BF16),
            pltpu.HBM((KF * CH, 2 * C), BF16),
            pltpu.VMEM((NCH, 1, CH), I32),
            pltpu.VMEM((NCH, 1, CH), I32),
            pltpu.VMEM((4, E), I32),
        ),
        [ANY, ANY, ANY, ANY, ANY, ANY],
        (VMEM, ANY, VMEM, VMEM, VMEM),
        [
            pltpu.SMEM((E,), I32),
            pltpu.VMEM((1, E), I32),
            pltpu.VMEM((SLOT, E), I32),
            pltpu.VMEM((1, E), I32),
            pltpu.VMEM((1, E), I32),
            pltpu.VMEM((NG, GR, C), BF16),
            pltpu.VMEM((NG + GCH, GR, C), BF16),
            pltpu.VMEM((KF * CH, 2 * C), BF16),
            dma((5,)),
            dma((LOADS,)),
            dma((KF,)),
        ],
        24,
        far(tile_counts.reshape(E)), far(tile_counts.T), far(tile_blocks.T), owner_row, label_row,
        far(tile_values.reshape(NG, GR, C)),
    )
    partial = local(
        margins_kernel, pltpu.VMEM((F, 1, E), F32), [VMEM, VMEM, VMEM, VMEM, VMEM, ANY], VMEM,
        [
            pltpu.VMEM((KF * CH, 2 * C), BF16),
            pltpu.VMEM((E + WIN, CH), F32),
            dma((KF,)),
        ],
        16,
        near(info), near(table), near(ids), near(ex), near(packed), far(over),
    )
    parts = lax.all_to_all(partial, "feat", 0, 0, tiled=True)
    payload = local(
        gradient_kernel, pltpu.VMEM((R, B // R + XR, C), BF16),
        [VMEM, VMEM, VMEM, VMEM, VMEM, ANY], VMEM,
        [
            pltpu.VMEM((KF * CH, 2 * C), BF16),
            pltpu.VMEM((B // 2, 2 * C), F32),
            pltpu.VMEM((E + WIN, C), F32),
            pltpu.VMEM((GROUP, 32, CH), BF16),
            dma((KF,)),
        ],
        16,
        near(info), near(parts), near(ids), near(ex), near(packed),
        far(over),
    )
    arrived = lax.all_to_all(payload, "rows", 0, 0, tiled=True)
    gradient, owned, loss = local(
        finish_kernel,
        (shape((B // R, C), F32), shape((1, E), F32), shape((1, 1), F32)),
        [VMEM], (VMEM, VMEM, VMEM), (), 8, near(arrived),
    )
    return owned.reshape(E), gradient, loss.reshape(())


def solution(mesh):
    in_specs = (
        P("rows", "feat", None),
        P("rows", "feat"),
        P("rows", "feat"),
        P("rows"),
        P("rows"),
        P(("feat", "rows"), None),
    )
    out_specs = (P("rows"), P(("feat", "rows"), None), P())
    return jax.shard_map(
        on_device, mesh=mesh, in_specs=in_specs, out_specs=out_specs, check_vma=False
    )
```

```python
import jax
import jax.numpy as jnp
from jax import lax
from jax.experimental import pallas as pl
from jax.experimental.pallas import tpu as pltpu
from jax.sharding import PartitionSpec as P

F32 = jnp.float32
BF16 = jnp.bfloat16
I32 = jnp.int32

E = 256
SLOT = 64
C = 128
B = 1024
R = 32
F = 8
OWN = 8
GR = 8
NG = E * SLOT // GR
CH = 512
GCH = CH // GR
NCH = NG // GCH
KA = 11
KF = NCH - KA
GROUP = 11
XR = 8
WIN = GCH + 8
FUSED = 4
EARLY = 2
LOADS = 4

VMEM = pl.BlockSpec(memory_space=pltpu.VMEM)
ANY = pl.BlockSpec(memory_space=pl.ANY)


def nt(a, b):
    return lax.dot_general(a, b, (((1,), (1,)), ((), ())), preferred_element_type=F32)


def nn(a, b):
    return lax.dot_general(a, b, (((1,), (0,)), ((), ())), preferred_element_type=F32)


def split3(x):
    hi = x.astype(BF16).astype(F32)
    mid = (x - hi).astype(BF16).astype(F32)
    lo = (x - hi - mid).astype(BF16).astype(F32)
    return hi, mid, lo


def iota(shape, dim):
    return lax.broadcasted_iota(I32, shape, dim)


def spread_weights(w_hbm, out_ref, w_ref, sem):
    pltpu.make_async_copy(w_hbm, w_ref, sem).start()
    pltpu.make_async_copy(w_hbm, w_ref, sem).wait()
    half = w_ref[...].astype(BF16)
    both = jnp.concatenate([half[0:16], half[16:32]], axis=1)
    out_ref[...] = jnp.broadcast_to(both[None], out_ref.shape)


def pack_tiles(
    flat_hbm, counts_hbm, blocks_hbm, owner_hbm, labels_hbm, values_hbm, near_ref, far_hbm, ids_ref,
    ex_ref, info_ref, counts_s, counts_ref, blocks_ref, owner_ref, labels_ref, values, packed, spill,
    small_sems, sems, out_sem
):
    part = NG // LOADS
    small = [
        pltpu.make_async_copy(src, dst, small_sems.at[i])
        for i, (src, dst) in enumerate(
            [
                (counts_hbm, counts_ref),
                (blocks_hbm, blocks_ref),
                (owner_hbm, owner_ref),
                (flat_hbm, counts_s),
                (labels_hbm, labels_ref),
            ]
        )
    ]
    loads = [
        pltpu.make_async_copy(
            values_hbm.at[pl.ds(i * part, part)], values.at[pl.ds(i * part, part)], sems.at[i]
        )
        for i in range(LOADS)
    ]
    for copy in small + loads:
        copy.start()
    for copy in small:
        copy.wait()

    counts = counts_ref[...]
    granules = lax.shift_right_logical(counts + (GR - 1), 3).astype(F32)
    spread = jnp.broadcast_to(granules, (E, E)).astype(BF16)
    up = iota((E, E), 0)
    across = iota((E, E), 1)
    first = nt((across < up).astype(F32).astype(BF16), spread)
    first = jnp.concatenate([first] * (CH // E), axis=1)
    before = (up < across).astype(F32).astype(BF16)
    start = nn(spread[0:16], before)
    start_hi = jnp.floor(start * (1.0 / 64.0))
    start_lo = start - 64.0 * start_hi
    row16 = iota((16, E), 0)
    tail = jnp.where(row16 == 0, start_hi, jnp.where(row16 == 1, start_lo, iota((16, E), 1).astype(F32)))
    ids = jnp.where(iota((SLOT, E), 0) < counts, blocks_ref[...], 2047)
    both = jnp.concatenate([lax.shift_right_logical(ids, 5), ids & 31], axis=0).astype(F32)
    table = jnp.concatenate([both, tail], axis=0)
    shifted = jnp.where(iota(table.shape, 1) == 0, 0.0, pltpu.roll(table, 1, 1))
    table = (table - shifted).astype(BF16)
    lane = iota((1, CH), 1)
    sub = iota((SLOT, CH), 0).astype(F32)
    total = jnp.sum(granules).astype(I32)
    chunks = lax.shift_right_logical(total + (GCH - 1), 6)

    hits = (iota((R, E), 0) == owner_ref[...]).astype(F32)
    earlier = nn(hits.astype(BF16), before)
    info_ref[0:1, :] = jnp.sum(hits * earlier, axis=0, keepdims=True).astype(I32)
    info_ref[1:2, :] = jnp.full((1, E), total, I32)
    info_ref[2:3, :] = owner_ref[...]
    info_ref[3:4, :] = labels_ref[...]

    def place(k, carry):
        pos = k * CH + lane
        gran = lax.shift_right_logical(pos, 3).astype(F32)
        x = nn(table, jnp.where(first <= gran, 1.0, 0.0).astype(BF16))
        slot = pos.astype(F32) - 8.0 * (64.0 * x[128:129] + x[129:130])
        code = 32.0 * x[0:64] + x[64:128]
        here = jnp.sum(jnp.where(sub == slot, code, 0.0), axis=0, keepdims=True).astype(I32)
        live = (pos < total * GR) & (here < B)
        ids_ref[k] = jnp.where(live, here, -1)
        ex_ref[k] = x[130:131].astype(I32)
        return carry


    def put_eight(i, off):
        for j in range(8):
            e = i * 8 + j
            packed[pl.ds(off, 8)] = values[pl.ds(e * 8, 8)]
            off = off + lax.shift_right_logical(counts_s[e] + (GR - 1), 3)
        return off

    def place_two(i, carry):
        place(2 * i, 0)
        return place(2 * i + 1, carry)

    def place_and_put(i, off):
        place(EARLY + i, 0)
        for j in range(FUSED):
            off = put_eight(FUSED * i + j, off)
        return off

    lax.fori_loop(0, EARLY // 2, place_two, 0)
    for copy in loads:
        copy.wait()
    lax.fori_loop(0, E // (8 * FUSED), place_and_put, 0)
    lax.fori_loop(EARLY + E // (8 * FUSED), chunks, place, 0)
    packed[pl.ds(total, GCH)] = jnp.zeros((GCH, GR, C), BF16)

    def widen(k, out, at):
        low, high = doubled(packed[pl.ds(k * GCH, GCH)].reshape(CH, C), ids_ref[k])
        span = pl.ds(pl.multiple_of(at * CH, CH), CH)
        out[span, 0:C] = low
        out[span, C : 2 * C] = high

    near = jnp.minimum(chunks, KA)

    def widen_pair(i, carry):
        for k in (2 * i, 2 * i + 1):
            k = jnp.minimum(k, full - 1)
            widen(jnp.minimum(k, near - 1), near_ref, k)
        return carry

    full = groups(near) * GROUP
    lax.fori_loop(0, lax.shift_right_logical(full + 1, 1), widen_pair, 0)

    def send(k):
        span = pl.ds(pl.multiple_of(k * CH, CH), CH)
        return pltpu.make_async_copy(spill.at[span], far_hbm.at[span], out_sem.at[k])

    def over(k, carry):
        widen(k + KA, spill, k)
        send(k).start()
        return carry

    def arrive(k, carry):
        send(k).wait()
        return carry

    lax.fori_loop(0, chunks - KA, over, 0)
    lax.fori_loop(0, chunks - KA, arrive, 0)


def groups(near):
    return lax.div(near + (GROUP - 1), GROUP)


def doubled(v, ids):
    top = jnp.broadcast_to(jnp.where((ids & 16) != 0, 1.0, 0.0), (8, CH)).T
    mask = jnp.broadcast_to(top[:, 0:1], (CH, C)).astype(BF16)
    high = v * mask
    return v - high, high


def scalar(row):
    return jnp.min(row[:, 0:128].astype(F32)).astype(I32)


def window(ex_ref, k):
    return pl.multiple_of(lax.shift_right_logical(scalar(ex_ref[k]), 3) * 8, 8)


def tiles(ref, k, n):
    return ref[pl.ds(pl.multiple_of(k * CH, CH), n * CH), :]


def each_chunk(info_ref, far_hbm, buf, sems, group, single):
    chunks = lax.shift_right_logical(scalar(info_ref[1:2, :]) + (GCH - 1), 6)
    near = jnp.minimum(chunks, KA)

    def fetch(k):
        span = pl.ds(pl.multiple_of(k * CH, CH), CH)
        return pltpu.make_async_copy(far_hbm.at[span], buf.at[span], sems.at[k])

    def start(k, carry):
        fetch(k).start()
        return carry

    lax.fori_loop(0, chunks - KA, start, 0)

    def inner(i, carry):
        group(i * GROUP, near)
        return carry

    lax.fori_loop(0, groups(near), inner, 0)

    def outer(k, carry):
        fetch(k).wait()
        single(k + KA, tiles(buf, k, 1))
        return carry

    lax.fori_loop(0, chunks - KA, outer, 0)


def margins_kernel(
    info_ref, w_ref, ids_ref, ex_ref, near_ref, far_hbm, out_ref, buf, acc, sems
):
    acc[...] = jnp.zeros_like(acc)
    rows = iota((WIN, CH), 0)
    sub8 = iota((8, CH), 0)

    def choose(k, score, live):
        ids = ids_ref[k]
        ids8 = jnp.broadcast_to(ids, (8, CH))
        pieces = [score[8 * i : 8 * i + 8, :] for i in range(B // 16)]
        half = 8
        while len(pieces) > 1:
            bit = (ids8 & half) != 0
            pieces = [jnp.where(bit, b, a) for a, b in zip(pieces[0::2], pieces[1::2])]
            half = 32 if half == 8 else 2 * half
        pick = jnp.sum(jnp.where(sub8 == (ids8 & 7), pieces[0], 0.0), axis=0, keepdims=True)
        pick = jnp.where((ids >= 0) & live, pick, 0.0)
        base = window(ex_ref, k)
        span = pl.ds(base, WIN)
        acc[span, :] += jnp.where(rows + base == ex_ref[k], pick, 0.0)

    def single(k, v):
        choose(k, nt(w_ref[...], v), True)

    def group(k, near):
        for j in range(GROUP):
            choose(jnp.minimum(k + j, near - 1), nt(w_ref[...], tiles(near_ref, k + j, 1)), k + j < near)

    each_chunk(info_ref, far_hbm, buf, sems, group, single)
    folded = acc[0:E, 0:C]
    for i in range(1, CH // C):
        folded = folded + acc[0:E, C * i : C * i + C]
    row = jnp.sum(folded.T, axis=0, keepdims=True)
    out_ref[...] = jnp.broadcast_to(row[None], out_ref.shape)


def gradient_kernel(
    info_ref, parts_ref, ids_ref, ex_ref, near_ref, far_hbm, out_ref, buf, acc, column_ref, sems
):
    acc[...] = jnp.zeros_like(acc)
    margin = jnp.sum(parts_ref[...].reshape(F, E), axis=0, keepdims=True)
    small_exp = jnp.exp(-jnp.abs(margin))
    label = info_ref[3:4, :].astype(F32)
    resid = jax.nn.sigmoid(margin) - label
    loss = jnp.sum(jnp.maximum(margin, 0.0) + jnp.log1p(small_exp) - label * margin)
    half = resid.astype(BF16).astype(F32)
    column_ref[0:E, :] = jnp.broadcast_to(half, (C, E)).T
    column_ref[E : E + WIN, :] = jnp.zeros((WIN, C), F32)

    owner_hit = iota((R, E), 0) == info_ref[2:3, :]
    rank = info_ref[0:1, :]
    lane_row = iota((C, E), 0)
    extra = jnp.zeros((R, C), F32)
    for i, piece in enumerate(split3(margin)):
        a = jnp.where(owner_hit, piece, 0.0).astype(BF16)
        b = jnp.where(lane_row == rank + OWN * i, 1.0, 0.0).astype(BF16)
        extra = extra + nt(a, b)
    lane = iota((R, C), 1)
    for i, piece in enumerate(split3(jnp.full((R, C), loss, F32))):
        extra = jnp.where(lane == 3 * OWN + i, piece, extra)
    out_ref[:, 32 : 32 + XR, :] = jnp.broadcast_to(extra[:, None, :], (R, XR, C)).astype(BF16)

    rows = iota((WIN, CH), 0)
    lo_rows = iota((16, CH), 0)

    def spread(k, live):
        ids = ids_ref[k]
        base = window(ex_ref, k)
        column = column_ref[pl.ds(base, WIN), :]
        column = jnp.concatenate([column] * (CH // C), axis=1)
        coef = jnp.sum(jnp.where(rows + base == ex_ref[k], column, 0.0), axis=0, keepdims=True)
        coef = jnp.where((ids >= 0) & live, coef, 0.0)
        low = jnp.where(lo_rows == (ids & 15), coef, 0.0).astype(BF16)
        high = lax.shift_right_arithmetic(ids, 5).astype(F32)
        high = jnp.broadcast_to(high, (16, CH)).astype(BF16)
        zero = jnp.zeros((), BF16)
        return jnp.concatenate([jnp.where(high == h, low, zero) for h in range(32)], axis=0)

    def single(k, v):
        acc[...] += nn(spread(k, True), v)

    def group(k, near):
        hot = [spread(jnp.minimum(k + j, near - 1), k + j < near) for j in range(GROUP)]
        acc[...] += nn(jnp.concatenate(hot, axis=1), tiles(near_ref, k, GROUP))

    each_chunk(info_ref, far_hbm, buf, sems, group, single)
    for i in range(2):
        out_ref[:, 16 * i : 16 * i + 16, :] = (
            acc[:, C * i : C * i + C].reshape(R, 16, C).astype(BF16)
        )


def finish_kernel(in_ref, grad_ref, owned_ref, loss_ref):
    total = in_ref[0, 0:32, :].astype(F32)
    for r in range(1, R):
        total = total + in_ref[r, 0:32, :].astype(F32)
    grad_ref[...] = total
    extra = in_ref[:, 32 : 32 + XR, :].astype(F32)[:, 0, :]
    src = iota((C, E), 0)
    pick = jnp.where((src < 3 * OWN) & ((src & 7) == (iota((C, E), 1) & 7)), 1.0, 0.0)
    wide = nn(extra.astype(BF16), pick.astype(BF16))
    own = lax.shift_right_logical(iota((R, E), 1), 3) == iota((R, E), 0)
    owned_ref[...] = jnp.sum(jnp.where(own, wide, 0.0), axis=0, keepdims=True)
    lane = iota((R, C), 1)
    keep = (lane >= 3 * OWN) & (lane < 3 * OWN + 3)
    total_loss = jnp.sum(jnp.where(keep, extra, 0.0), keepdims=True)
    loss_ref[...] = total_loss * (1.0 / (E * R))


def local(body, out_shapes, in_specs, out_specs, scratch, limit, *args):
    return pl.pallas_call(
        body,
        out_shape=out_shapes,
        in_specs=in_specs,
        out_specs=out_specs,
        scratch_shapes=scratch,
        compiler_params=pltpu.CompilerParams(vmem_limit_bytes=limit << 20),
    )(*args)


def near(x):
    return pltpu.with_memory_space_constraint(x, pltpu.VMEM)


def far(x):
    return pltpu.with_memory_space_constraint(x, pltpu.HBM)


def on_device(tile_values, tile_blocks, tile_counts, labels, owner_rank, weights):
    shape = jax.ShapeDtypeStruct
    dma = pltpu.SemaphoreType.DMA
    spread = local(
        spread_weights, pltpu.VMEM((R, B // (2 * R), 2 * C), BF16), [ANY], VMEM,
        [pltpu.VMEM((B // R, C), F32), dma(())], 4, far(weights),
    )
    table = lax.all_to_all(spread, "rows", 0, 0, tiled=True).reshape(B // 2, 2 * C)
    owner_row = far(owner_rank.reshape(1, E))
    label_row = far(labels.reshape(1, E))
    packed, over, ids, ex, info = local(
        pack_tiles,
        (
            pltpu.VMEM((KA * CH, 2 * C), BF16),
            pltpu.HBM((KF * CH, 2 * C), BF16),
            pltpu.VMEM((NCH, 1, CH), I32),
            pltpu.VMEM((NCH, 1, CH), I32),
            pltpu.VMEM((4, E), I32),
        ),
        [ANY, ANY, ANY, ANY, ANY, ANY],
        (VMEM, ANY, VMEM, VMEM, VMEM),
        [
            pltpu.SMEM((E,), I32),
            pltpu.VMEM((1, E), I32),
            pltpu.VMEM((SLOT, E), I32),
            pltpu.VMEM((1, E), I32),
            pltpu.VMEM((1, E), I32),
            pltpu.VMEM((NG, GR, C), BF16),
            pltpu.VMEM((NG + GCH, GR, C), BF16),
            pltpu.VMEM((KF * CH, 2 * C), BF16),
            dma((5,)),
            dma((LOADS,)),
            dma((KF,)),
        ],
        24,
        far(tile_counts.reshape(E)), far(tile_counts.T), far(tile_blocks.T), owner_row, label_row,
        far(tile_values.reshape(NG, GR, C)),
    )
    partial = local(
        margins_kernel, pltpu.VMEM((F, 1, E), F32), [VMEM, VMEM, VMEM, VMEM, VMEM, ANY], VMEM,
        [
            pltpu.VMEM((KF * CH, 2 * C), BF16),
            pltpu.VMEM((E + WIN, CH), F32),
            dma((KF,)),
        ],
        16,
        near(info), near(table), near(ids), near(ex), near(packed), far(over),
    )
    parts = lax.all_to_all(partial, "feat", 0, 0, tiled=True)
    payload = local(
        gradient_kernel, pltpu.VMEM((R, B // R + XR, C), BF16),
        [VMEM, VMEM, VMEM, VMEM, VMEM, ANY], VMEM,
        [
            pltpu.VMEM((KF * CH, 2 * C), BF16),
            pltpu.VMEM((B // 2, 2 * C), F32),
            pltpu.VMEM((E + WIN, C), F32),
            dma((KF,)),
        ],
        16,
        near(info), near(parts), near(ids), near(ex), near(packed),
        far(over),
    )
    arrived = lax.all_to_all(payload, "rows", 0, 0, tiled=True)
    gradient, owned, loss = local(
        finish_kernel,
        (shape((B // R, C), F32), shape((1, E), F32), shape((1, 1), F32)),
        [VMEM], (VMEM, VMEM, VMEM), (), 8, near(arrived),
    )
    return owned.reshape(E), gradient, loss.reshape(())


def solution(mesh):
    in_specs = (
        P("rows", "feat", None),
        P("rows", "feat"),
        P("rows", "feat"),
        P("rows"),
        P("rows"),
        P(("feat", "rows"), None),
    )
    out_specs = (P("rows"), P(("feat", "rows"), None), P())
    return jax.shard_map(
        on_device, mesh=mesh, in_specs=in_specs, out_specs=out_specs, check_vma=False
    )
```

```python
import jax
import jax.numpy as jnp
from jax import lax
from jax.experimental import pallas as pl
from jax.experimental.pallas import tpu as pltpu
from jax.sharding import PartitionSpec as P

F32 = jnp.float32
BF16 = jnp.bfloat16
I32 = jnp.int32

E = 256
SLOT = 64
C = 128
B = 1024
R = 32
F = 8
OWN = 8
GR = 8
NG = E * SLOT // GR
CH = 512
GCH = CH // GR
NCH = NG // GCH
KA = 11
KF = NCH - KA
XR = 8
WIN = GCH + 8
FUSED = 4
EARLY = KA - 8
LOADS = 4

VMEM = pl.BlockSpec(memory_space=pltpu.VMEM)
ANY = pl.BlockSpec(memory_space=pl.ANY)


def nt(a, b):
    return lax.dot_general(a, b, (((1,), (1,)), ((), ())), preferred_element_type=F32)


def nn(a, b):
    return lax.dot_general(a, b, (((1,), (0,)), ((), ())), preferred_element_type=F32)


def split3(x):
    hi = x.astype(BF16).astype(F32)
    mid = (x - hi).astype(BF16).astype(F32)
    lo = (x - hi - mid).astype(BF16).astype(F32)
    return hi, mid, lo


def iota(shape, dim):
    return lax.broadcasted_iota(I32, shape, dim)


def spread_weights(w_hbm, out_ref, w_ref, sem):
    pltpu.make_async_copy(w_hbm, w_ref, sem).start()
    pltpu.make_async_copy(w_hbm, w_ref, sem).wait()
    half = w_ref[...].astype(BF16)
    both = jnp.concatenate([half[0:16], half[16:32]], axis=1)
    out_ref[...] = jnp.broadcast_to(both[None], out_ref.shape)


def pack_tiles(
    flat_hbm, counts_hbm, blocks_hbm, owner_hbm, labels_hbm, values_hbm, near_ref, far_hbm, ids_ref,
    ex_ref, info_ref, counts_s, counts_ref, blocks_ref, owner_ref, labels_ref, values, packed, spill,
    small_sems, sems, out_sem
):
    part = NG // LOADS
    small = [
        pltpu.make_async_copy(src, dst, small_sems.at[i])
        for i, (src, dst) in enumerate(
            [
                (counts_hbm, counts_ref),
                (blocks_hbm, blocks_ref),
                (owner_hbm, owner_ref),
                (flat_hbm, counts_s),
                (labels_hbm, labels_ref),
            ]
        )
    ]
    loads = [
        pltpu.make_async_copy(
            values_hbm.at[pl.ds(i * part, part)], values.at[pl.ds(i * part, part)], sems.at[i]
        )
        for i in range(LOADS)
    ]
    for copy in small + loads:
        copy.start()
    for copy in small:
        copy.wait()

    counts = counts_ref[...]
    granules = lax.shift_right_logical(counts + (GR - 1), 3).astype(F32)
    spread = jnp.broadcast_to(granules, (E, E)).astype(BF16)
    up = iota((E, E), 0)
    across = iota((E, E), 1)
    first = nt((across < up).astype(F32).astype(BF16), spread)
    first = jnp.concatenate([first] * (CH // E), axis=1)
    before = (up < across).astype(F32).astype(BF16)
    start = nn(spread[0:16], before)
    start_hi = jnp.floor(start * (1.0 / 64.0))
    start_lo = start - 64.0 * start_hi
    row16 = iota((16, E), 0)
    tail = jnp.where(row16 == 0, start_hi, jnp.where(row16 == 1, start_lo, iota((16, E), 1).astype(F32)))
    ids = jnp.where(iota((SLOT, E), 0) < counts, blocks_ref[...], 2047)
    both = jnp.concatenate([lax.shift_right_logical(ids, 5), ids & 31], axis=0).astype(F32)
    table = jnp.concatenate([both, tail], axis=0)
    shifted = jnp.where(iota(table.shape, 1) == 0, 0.0, pltpu.roll(table, 1, 1))
    table = (table - shifted).astype(BF16)
    lane = iota((1, CH), 1)
    sub = iota((SLOT, CH), 0).astype(F32)
    total = jnp.sum(granules).astype(I32)
    chunks = lax.shift_right_logical(total + (GCH - 1), 6)

    hits = (iota((R, E), 0) == owner_ref[...]).astype(F32)
    earlier = nn(hits.astype(BF16), before)
    info_ref[0:1, :] = jnp.sum(hits * earlier, axis=0, keepdims=True).astype(I32)
    info_ref[1:2, :] = jnp.full((1, E), total, I32)
    info_ref[2:3, :] = owner_ref[...]
    info_ref[3:4, :] = labels_ref[...]

    def place(k, carry):
        pos = k * CH + lane
        gran = lax.shift_right_logical(pos, 3).astype(F32)
        x = nn(table, jnp.where(first <= gran, 1.0, 0.0).astype(BF16))
        slot = pos.astype(F32) - 8.0 * (64.0 * x[128:129] + x[129:130])
        code = 32.0 * x[0:64] + x[64:128]
        here = jnp.sum(jnp.where(sub == slot, code, 0.0), axis=0, keepdims=True).astype(I32)
        live = (pos < total * GR) & (here < B)
        ids_ref[k] = jnp.where(live, here, -1)
        ex_ref[k] = x[130:131].astype(I32)
        return carry


    def put_eight(i, off):
        for j in range(8):
            e = i * 8 + j
            packed[pl.ds(off, 8)] = values[pl.ds(e * 8, 8)]
            off = off + lax.shift_right_logical(counts_s[e] + (GR - 1), 3)
        return off

    def place_and_put(i, off):
        place(EARLY + i, 0)
        for j in range(FUSED):
            off = put_eight(FUSED * i + j, off)
        return off

    for k in range(EARLY):
        place(k, 0)
    for copy in loads:
        copy.wait()
    lax.fori_loop(0, E // (8 * FUSED), place_and_put, 0)
    lax.fori_loop(EARLY + E // (8 * FUSED), chunks, place, 0)
    packed[pl.ds(total, GCH)] = jnp.zeros((GCH, GR, C), BF16)

    def widen(k, out, at):
        low, high = doubled(packed[pl.ds(k * GCH, GCH)].reshape(CH, C), ids_ref[k])
        span = pl.ds(pl.multiple_of(at * CH, CH), CH)
        out[span, 0:C] = low
        out[span, C : 2 * C] = high

    near = jnp.minimum(chunks, KA)

    def widen_pair(i, carry):
        for k in (2 * i, 2 * i + 1):
            widen(jnp.minimum(k, near - 1), near_ref, k)
        return carry

    lax.fori_loop(0, KA // 2, widen_pair, 0)
    for k in range(KA // 2 * 2, KA):
        widen(jnp.minimum(k, near - 1), near_ref, k)

    def send(k):
        span = pl.ds(pl.multiple_of(k * CH, CH), CH)
        return pltpu.make_async_copy(spill.at[span], far_hbm.at[span], out_sem.at[k])

    def over(k, carry):
        widen(k + KA, spill, k)
        send(k).start()
        return carry

    def arrive(k, carry):
        send(k).wait()
        return carry

    lax.fori_loop(0, chunks - KA, over, 0)
    lax.fori_loop(0, chunks - KA, arrive, 0)


def doubled(v, ids):
    top = jnp.broadcast_to(jnp.where((ids & 16) != 0, 1.0, 0.0), (8, CH)).T
    mask = jnp.broadcast_to(top[:, 0:1], (CH, C)).astype(BF16)
    high = v * mask
    return v - high, high


def scalar(row):
    return jnp.min(row[:, 0:128].astype(F32)).astype(I32)


def window(ex_ref, k):
    return pl.multiple_of(lax.shift_right_logical(scalar(ex_ref[k]), 3) * 8, 8)


def tiles(ref, k, n):
    if isinstance(k, int):
        return ref[k * CH : (k + n) * CH, :]
    return ref[pl.ds(pl.multiple_of(k * CH, CH), n * CH), :]


def fold(x):
    return sum(x[:, C * i : C * i + C] for i in range(1, CH // C)) + x[:, 0:C]


def far_chunks(info_ref, far_hbm, buf, sems, near_work, far_work):
    chunks = lax.shift_right_logical(scalar(info_ref[1:2, :]) + (GCH - 1), 6)

    def fetch(k):
        span = pl.ds(pl.multiple_of(k * CH, CH), CH)
        return pltpu.make_async_copy(far_hbm.at[span], buf.at[span], sems.at[k])

    def start(k, carry):
        fetch(k).start()
        return carry

    def outer(k, carry):
        fetch(k).wait()
        far_work(k + KA, tiles(buf, k, 1))
        return carry

    near_work()
    lax.fori_loop(0, chunks - KA, start, 0)
    lax.fori_loop(0, chunks - KA, outer, 0)


def margins_kernel(
    info_ref, w_ref, ids_ref, ex_ref, near_ref, far_hbm, out_ref, buf, acc, sems
):
    acc[...] = jnp.zeros_like(acc)
    rows = iota((WIN, CH), 0)
    sub8 = iota((8, CH), 0)

    def choose(k, score):
        ids = ids_ref[k]
        ids8 = jnp.broadcast_to(ids, (8, CH))
        pieces = [score[8 * i : 8 * i + 8, :] for i in range(B // 16)]
        half = 8
        while len(pieces) > 1:
            bit = (ids8 & half) != 0
            pieces = [jnp.where(bit, b, a) for a, b in zip(pieces[0::2], pieces[1::2])]
            half = 32 if half == 8 else 2 * half
        pick = jnp.sum(jnp.where(sub8 == (ids8 & 7), pieces[0], 0.0), axis=0, keepdims=True)
        pick = jnp.where(ids >= 0, pick, 0.0)
        base = window(ex_ref, k)
        span = pl.ds(base, WIN)
        mine = jnp.where(rows + base == ex_ref[k], pick, 0.0)
        acc[span, :] += fold(mine)

    def near_work():
        for k in range(KA):
            choose(k, nt(w_ref[...], tiles(near_ref, k, 1)))

    def far_work(k, v):
        choose(k, nt(w_ref[...], v))

    far_chunks(info_ref, far_hbm, buf, sems, near_work, far_work)
    row = jnp.sum(acc[0:E, :].T, axis=0, keepdims=True)
    out_ref[...] = jnp.broadcast_to(row[None], out_ref.shape)


def gradient_kernel(
    info_ref, parts_ref, ids_ref, ex_ref, near_ref, far_hbm, out_ref, buf, acc, column_ref, sems
):
    margin = jnp.sum(parts_ref[...].reshape(F, E), axis=0, keepdims=True)
    small_exp = jnp.exp(-jnp.abs(margin))
    label = info_ref[3:4, :].astype(F32)
    resid = jax.nn.sigmoid(margin) - label
    loss = jnp.maximum(margin, 0.0) + jnp.log1p(small_exp) - label * margin
    loss = jnp.broadcast_to(jnp.sum(loss, axis=1, keepdims=True), (R, C))
    half = resid.astype(BF16).astype(F32)
    column_ref[0:E, :] = jnp.broadcast_to(half, (C, E)).T
    column_ref[E : E + WIN, :] = jnp.zeros((WIN, C), F32)

    owner_hit = iota((R, E), 0) == info_ref[2:3, :]
    rank = info_ref[0:1, :]
    lane_row = iota((C, E), 0)
    extra = jnp.zeros((R, C), F32)
    for i, piece in enumerate(split3(margin)):
        a = jnp.where(owner_hit, piece, 0.0).astype(BF16)
        b = jnp.where(lane_row == rank + OWN * i, 1.0, 0.0).astype(BF16)
        extra = extra + nt(a, b)
    lane = iota((R, C), 1)
    for i, piece in enumerate(split3(loss)):
        extra = jnp.where(lane == 3 * OWN + i, piece, extra)
    out_ref[:, 32 : 32 + XR, :] = jnp.broadcast_to(extra[:, None, :], (R, XR, C)).astype(BF16)

    rows = iota((WIN, CH), 0)
    lo_rows = iota((16, CH), 0)

    def spread(k):
        ids = ids_ref[k]
        base = window(ex_ref, k)
        column = column_ref[pl.ds(base, WIN), :]
        column = jnp.concatenate([column] * (CH // C), axis=1)
        coef = jnp.sum(jnp.where(rows + base == ex_ref[k], column, 0.0), axis=0, keepdims=True)
        coef = jnp.where(ids >= 0, coef, 0.0)
        low = jnp.where(lo_rows == (ids & 15), coef, 0.0).astype(BF16)
        high = lax.shift_right_arithmetic(ids, 5).astype(F32)
        high = jnp.broadcast_to(high, (16, CH)).astype(BF16)
        zero = jnp.zeros((), BF16)
        return jnp.concatenate([jnp.where(high == h, low, zero) for h in range(32)], axis=0)

    def near_work():
        hot = jnp.concatenate([spread(k) for k in range(KA)], axis=1)
        acc[...] = nn(hot, tiles(near_ref, 0, KA))

    def far_work(k, v):
        acc[...] += nn(spread(k), v)

    far_chunks(info_ref, far_hbm, buf, sems, near_work, far_work)
    for i in range(2):
        out_ref[:, 16 * i : 16 * i + 16, :] = (
            acc[:, C * i : C * i + C].reshape(R, 16, C).astype(BF16)
        )


def finish_kernel(in_ref, grad_ref, owned_ref, loss_ref):
    total = in_ref[0, 0:32, :].astype(F32)
    for r in range(1, R):
        total = total + in_ref[r, 0:32, :].astype(F32)
    grad_ref[...] = total
    extra = in_ref[:, 32 : 32 + XR, :].astype(F32)[:, 0, :]
    src = iota((C, E), 0)
    pick = jnp.where((src < 3 * OWN) & ((src & 7) == (iota((C, E), 1) & 7)), 1.0, 0.0)
    wide = nn(extra.astype(BF16), pick.astype(BF16))
    own = lax.shift_right_logical(iota((R, E), 1), 3) == iota((R, E), 0)
    owned_ref[...] = jnp.sum(jnp.where(own, wide, 0.0), axis=0, keepdims=True)
    lane = iota((R, C), 1)
    keep = (lane >= 3 * OWN) & (lane < 3 * OWN + 3)
    total_loss = jnp.sum(jnp.where(keep, extra, 0.0), keepdims=True)
    loss_ref[...] = total_loss * (1.0 / (E * R))


def local(body, out_shapes, in_specs, out_specs, scratch, limit, *args):
    return pl.pallas_call(
        body,
        out_shape=out_shapes,
        in_specs=in_specs,
        out_specs=out_specs,
        scratch_shapes=scratch,
        compiler_params=pltpu.CompilerParams(vmem_limit_bytes=limit << 20),
    )(*args)


def near(x):
    return pltpu.with_memory_space_constraint(x, pltpu.VMEM)


def far(x):
    return pltpu.with_memory_space_constraint(x, pltpu.HBM)


def on_device(tile_values, tile_blocks, tile_counts, labels, owner_rank, weights):
    shape = jax.ShapeDtypeStruct
    dma = pltpu.SemaphoreType.DMA
    spread = local(
        spread_weights, pltpu.VMEM((R, B // (2 * R), 2 * C), BF16), [ANY], VMEM,
        [pltpu.VMEM((B // R, C), F32), dma(())], 4, far(weights),
    )
    table = lax.all_to_all(spread, "rows", 0, 0, tiled=True).reshape(B // 2, 2 * C)
    owner_row = far(owner_rank.reshape(1, E))
    label_row = far(labels.reshape(1, E))
    packed, over, ids, ex, info = local(
        pack_tiles,
        (
            pltpu.VMEM((KA * CH, 2 * C), BF16),
            pltpu.HBM((KF * CH, 2 * C), BF16),
            pltpu.VMEM((NCH, 1, CH), I32),
            pltpu.VMEM((NCH, 1, CH), I32),
            pltpu.VMEM((4, E), I32),
        ),
        [ANY, ANY, ANY, ANY, ANY, ANY],
        (VMEM, ANY, VMEM, VMEM, VMEM),
        [
            pltpu.SMEM((E,), I32),
            pltpu.VMEM((1, E), I32),
            pltpu.VMEM((SLOT, E), I32),
            pltpu.VMEM((1, E), I32),
            pltpu.VMEM((1, E), I32),
            pltpu.VMEM((NG, GR, C), BF16),
            pltpu.VMEM((NG + GCH, GR, C), BF16),
            pltpu.VMEM((KF * CH, 2 * C), BF16),
            dma((5,)),
            dma((LOADS,)),
            dma((KF,)),
        ],
        24,
        far(tile_counts.reshape(E)), far(tile_counts.T), far(tile_blocks.T), owner_row, label_row,
        far(tile_values.reshape(NG, GR, C)),
    )
    partial = local(
        margins_kernel, pltpu.VMEM((F, 1, E), F32), [VMEM, VMEM, VMEM, VMEM, VMEM, ANY], VMEM,
        [
            pltpu.VMEM((KF * CH, 2 * C), BF16),
            pltpu.VMEM((E + WIN, C), F32),
            dma((KF,)),
        ],
        16,
        near(info), near(table), near(ids), near(ex), near(packed), far(over),
    )
    parts = lax.all_to_all(partial, "feat", 0, 0, tiled=True)
    payload = local(
        gradient_kernel, pltpu.VMEM((R, B // R + XR, C), BF16),
        [VMEM, VMEM, VMEM, VMEM, VMEM, ANY], VMEM,
        [
            pltpu.VMEM((KF * CH, 2 * C), BF16),
            pltpu.VMEM((B // 2, 2 * C), F32),
            pltpu.VMEM((E + WIN, C), F32),
            dma((KF,)),
        ],
        16,
        near(info), near(parts), near(ids), near(ex), near(packed),
        far(over),
    )
    arrived = lax.all_to_all(payload, "rows", 0, 0, tiled=True)
    gradient, owned, loss = local(
        finish_kernel,
        (shape((B // R, C), F32), shape((1, E), F32), shape((1, 1), F32)),
        [VMEM], (VMEM, VMEM, VMEM), (), 8, near(arrived),
    )
    return owned.reshape(E), gradient, loss.reshape(())


def solution(mesh):
    in_specs = (
        P("rows", "feat", None),
        P("rows", "feat"),
        P("rows", "feat"),
        P("rows"),
        P("rows"),
        P(("feat", "rows"), None),
    )
    out_specs = (P("rows"), P(("feat", "rows"), None), P())
    return jax.shard_map(
        on_device, mesh=mesh, in_specs=in_specs, out_specs=out_specs, check_vma=False
    )
```

```python
import jax
import jax.numpy as jnp
from jax import lax
from jax.experimental import pallas as pl
from jax.experimental.pallas import tpu as pltpu
from jax.sharding import PartitionSpec as P

F32 = jnp.float32
BF16 = jnp.bfloat16
I32 = jnp.int32

E = 256
SLOT = 64
C = 128
B = 1024
R = 32
F = 8
OWN = 8
GR = 8
NG = E * SLOT // GR
CH = 512
GCH = CH // GR
NCH = NG // GCH
KA = 11
KF = NCH - KA
XR = 8
WIN = GCH + 8
FUSED = 4
EARLY = KA - 8
LOADS = 4

VMEM = pl.BlockSpec(memory_space=pltpu.VMEM)
ANY = pl.BlockSpec(memory_space=pl.ANY)


def nt(a, b):
    return lax.dot_general(a, b, (((1,), (1,)), ((), ())), preferred_element_type=F32)


def nn(a, b):
    return lax.dot_general(a, b, (((1,), (0,)), ((), ())), preferred_element_type=F32)


def split3(x):
    hi = x.astype(BF16).astype(F32)
    mid = (x - hi).astype(BF16).astype(F32)
    lo = (x - hi - mid).astype(BF16).astype(F32)
    return hi, mid, lo


def iota(shape, dim):
    return lax.broadcasted_iota(I32, shape, dim)


def spread_weights(w_hbm, out_ref, w_ref, sem):
    pltpu.make_async_copy(w_hbm, w_ref, sem).start()
    pltpu.make_async_copy(w_hbm, w_ref, sem).wait()
    half = w_ref[...].astype(BF16)
    both = jnp.concatenate([half[0:16], half[16:32]], axis=1)
    out_ref[...] = jnp.broadcast_to(both[None], out_ref.shape)


def pack_tiles(
    flat_hbm, counts_hbm, blocks_hbm, owner_hbm, labels_hbm, values_hbm, near_ref, far_hbm, ids_ref,
    ex_ref, info_ref, counts_s, counts_ref, blocks_ref, owner_ref, labels_ref, values, packed, spill,
    small_sems, sems, out_sem
):
    part = NG // LOADS
    small = [
        pltpu.make_async_copy(src, dst, small_sems.at[i])
        for i, (src, dst) in enumerate(
            [
                (counts_hbm, counts_ref),
                (blocks_hbm, blocks_ref),
                (owner_hbm, owner_ref),
                (flat_hbm, counts_s),
                (labels_hbm, labels_ref),
            ]
        )
    ]
    loads = [
        pltpu.make_async_copy(
            values_hbm.at[pl.ds(i * part, part)], values.at[pl.ds(i * part, part)], sems.at[i]
        )
        for i in range(LOADS)
    ]
    for copy in small + loads:
        copy.start()
    for copy in small:
        copy.wait()

    counts = counts_ref[...]
    granules = lax.shift_right_logical(counts + (GR - 1), 3).astype(F32)
    spread = jnp.broadcast_to(granules, (E, E)).astype(BF16)
    up = iota((E, E), 0)
    across = iota((E, E), 1)
    first = nt((across < up).astype(F32).astype(BF16), spread)
    first = jnp.concatenate([first] * (CH // E), axis=1)
    before = (up < across).astype(F32).astype(BF16)
    start = nn(spread[0:16], before)
    start_hi = jnp.floor(start * (1.0 / 64.0))
    start_lo = start - 64.0 * start_hi
    row16 = iota((16, E), 0)
    tail = jnp.where(row16 == 0, start_hi, jnp.where(row16 == 1, start_lo, iota((16, E), 1).astype(F32)))
    ids = jnp.where(iota((SLOT, E), 0) < counts, blocks_ref[...], 2047)
    both = jnp.concatenate([lax.shift_right_logical(ids, 5), ids & 31], axis=0).astype(F32)
    table = jnp.concatenate([both, tail], axis=0)
    shifted = jnp.where(iota(table.shape, 1) == 0, 0.0, pltpu.roll(table, 1, 1))
    table = (table - shifted).astype(BF16)
    lane = iota((1, CH), 1)
    sub = iota((SLOT, CH), 0).astype(F32)
    total = jnp.sum(granules).astype(I32)
    chunks = lax.shift_right_logical(total + (GCH - 1), 6)

    hits = (iota((R, E), 0) == owner_ref[...]).astype(F32)
    earlier = nn(hits.astype(BF16), before)
    info_ref[0:1, :] = jnp.sum(hits * earlier, axis=0, keepdims=True).astype(I32)
    info_ref[1:2, :] = jnp.full((1, E), total, I32)
    info_ref[2:3, :] = owner_ref[...]
    info_ref[3:4, :] = labels_ref[...]

    def place(k, carry):
        pos = k * CH + lane
        gran = lax.shift_right_logical(pos, 3).astype(F32)
        x = nn(table, jnp.where(first <= gran, 1.0, 0.0).astype(BF16))
        slot = pos.astype(F32) - 8.0 * (64.0 * x[128:129] + x[129:130])
        code = 32.0 * x[0:64] + x[64:128]
        here = jnp.sum(jnp.where(sub == slot, code, 0.0), axis=0, keepdims=True).astype(I32)
        live = (pos < total * GR) & (here < B)
        ids_ref[k] = jnp.where(live, here, -1)
        ex_ref[k] = x[130:131].astype(I32)
        return carry


    def put_eight(i, off):
        for j in range(8):
            e = i * 8 + j
            packed[pl.ds(off, 8)] = values[pl.ds(e * 8, 8)]
            off = off + lax.shift_right_logical(counts_s[e] + (GR - 1), 3)
        return off

    def place_and_put(i, off):
        place(EARLY + i, 0)
        for j in range(FUSED):
            off = put_eight(FUSED * i + j, off)
        return off

    for k in range(EARLY):
        place(k, 0)
    for copy in loads:
        copy.wait()
    lax.fori_loop(0, E // (8 * FUSED), place_and_put, 0)
    lax.fori_loop(EARLY + E // (8 * FUSED), chunks, place, 0)
    packed[pl.ds(total, GCH)] = jnp.zeros((GCH, GR, C), BF16)

    def widen(k, out, at):
        low, high = doubled(packed[pl.ds(k * GCH, GCH)].reshape(CH, C), ids_ref[k])
        span = pl.ds(pl.multiple_of(at * CH, CH), CH)
        out[span, 0:C] = low
        out[span, C : 2 * C] = high

    near = jnp.minimum(chunks, KA)

    def widen_pair(i, carry):
        for k in (2 * i, 2 * i + 1):
            widen(jnp.minimum(k, near - 1), near_ref, k)
        return carry

    lax.fori_loop(0, KA // 2, widen_pair, 0)
    for k in range(KA // 2 * 2, KA):
        widen(jnp.minimum(k, near - 1), near_ref, k)

    def send(k):
        span = pl.ds(pl.multiple_of(k * CH, CH), CH)
        return pltpu.make_async_copy(spill.at[span], far_hbm.at[span], out_sem.at[k])

    def over(k, carry):
        widen(k + KA, spill, k)
        send(k).start()
        return carry

    def arrive(k, carry):
        send(k).wait()
        return carry

    lax.fori_loop(0, chunks - KA, over, 0)
    lax.fori_loop(0, chunks - KA, arrive, 0)


def doubled(v, ids):
    top = jnp.broadcast_to(jnp.where((ids & 16) != 0, 1.0, 0.0), (8, CH)).T
    mask = jnp.broadcast_to(top[:, 0:1], (CH, C)).astype(BF16)
    high = v * mask
    return v - high, high


def scalar(row):
    return jnp.min(row[:, 0:128].astype(F32)).astype(I32)


def window(ex_ref, k):
    return pl.multiple_of(lax.shift_right_logical(scalar(ex_ref[k]), 3) * 8, 8)


def tiles(ref, k, n):
    if isinstance(k, int):
        return ref[k * CH : (k + n) * CH, :]
    return ref[pl.ds(pl.multiple_of(k * CH, CH), n * CH), :]


def fold(x):
    return sum(x[:, C * i : C * i + C] for i in range(1, CH // C)) + x[:, 0:C]


def far_chunks(info_ref, far_hbm, buf, sems, near_work, far_work):
    chunks = lax.shift_right_logical(scalar(info_ref[1:2, :]) + (GCH - 1), 6)

    def fetch(k):
        span = pl.ds(pl.multiple_of(k * CH, CH), CH)
        return pltpu.make_async_copy(far_hbm.at[span], buf.at[span], sems.at[k])

    def start(k, carry):
        fetch(k).start()
        return carry

    def outer(k, carry):
        fetch(k).wait()
        far_work(k + KA, tiles(buf, k, 1))
        return carry

    near_work()
    lax.fori_loop(0, chunks - KA, start, 0)
    lax.fori_loop(0, chunks - KA, outer, 0)


def margins_kernel(
    info_ref, w_ref, ids_ref, ex_ref, near_ref, far_hbm, out_ref, buf, acc, sems
):
    acc[...] = jnp.zeros_like(acc)
    rows = iota((WIN, CH), 0)
    sub8 = iota((8, CH), 0)

    def choose(k, score):
        ids = ids_ref[k]
        ids8 = jnp.broadcast_to(ids, (8, CH))
        pieces = [score[8 * i : 8 * i + 8, :] for i in range(B // 16)]
        half = 8
        while len(pieces) > 1:
            bit = (ids8 & half) != 0
            pieces = [jnp.where(bit, b, a) for a, b in zip(pieces[0::2], pieces[1::2])]
            half = 32 if half == 8 else 2 * half
        pick = jnp.sum(jnp.where(sub8 == (ids8 & 7), pieces[0], 0.0), axis=0, keepdims=True)
        pick = jnp.where(ids >= 0, pick, 0.0)
        base = window(ex_ref, k)
        span = pl.ds(base, WIN)
        mine = jnp.where(rows + base == ex_ref[k], pick, 0.0)
        acc[span, :] += fold(mine)

    def near_work():
        for k in range(KA):
            choose(k, nt(w_ref[...], tiles(near_ref, k, 1)))

    def far_work(k, v):
        choose(k, nt(w_ref[...], v))

    far_chunks(info_ref, far_hbm, buf, sems, near_work, far_work)
    row = jnp.sum(acc[0:E, :].T, axis=0, keepdims=True)
    out_ref[...] = jnp.broadcast_to(row[None], out_ref.shape)


def gradient_kernel(
    info_ref, parts_ref, ids_ref, ex_ref, near_ref, far_hbm, out_ref, buf, acc, column_ref, sems
):
    margin = jnp.sum(parts_ref[...].reshape(F, E), axis=0, keepdims=True)
    small_exp = jnp.exp(-jnp.abs(margin))
    label = info_ref[3:4, :].astype(F32)
    resid = jax.nn.sigmoid(margin) - label
    loss = jnp.maximum(margin, 0.0) + jnp.log1p(small_exp) - label * margin
    loss = jnp.broadcast_to(jnp.sum(loss, axis=1, keepdims=True), (R, C))
    half = resid.astype(BF16).astype(F32)
    column_ref[0:E, :] = jnp.broadcast_to(half, (C, E)).T
    column_ref[E : E + WIN, :] = jnp.zeros((WIN, C), F32)

    owner_hit = iota((R, E), 0) == info_ref[2:3, :]
    rank = info_ref[0:1, :]
    lane_row = iota((C, E), 0)
    extra = jnp.zeros((R, C), F32)
    for i, piece in enumerate(split3(margin)):
        a = jnp.where(owner_hit, piece, 0.0).astype(BF16)
        b = jnp.where(lane_row == rank + OWN * i, 1.0, 0.0).astype(BF16)
        extra = extra + nt(a, b)
    lane = iota((R, C), 1)
    for i, piece in enumerate(split3(loss)):
        extra = jnp.where(lane == 3 * OWN + i, piece, extra)
    out_ref[:, 32 : 32 + XR, :] = jnp.broadcast_to(extra[:, None, :], (R, XR, C)).astype(BF16)

    rows = iota((WIN, CH), 0)
    lo_rows = iota((16, CH), 0)

    def spread(k):
        ids = ids_ref[k]
        base = window(ex_ref, k)
        column = column_ref[pl.ds(base, WIN), :]
        column = jnp.concatenate([column] * (CH // C), axis=1)
        coef = jnp.sum(jnp.where(rows + base == ex_ref[k], column, 0.0), axis=0, keepdims=True)
        coef = jnp.where(ids >= 0, coef, 0.0)
        low = jnp.where(lo_rows == (ids & 15), coef, 0.0).astype(BF16)
        high = lax.shift_right_arithmetic(ids, 5).astype(F32)
        high = jnp.broadcast_to(high, (16, CH)).astype(BF16)
        zero = jnp.zeros((), BF16)
        return jnp.concatenate([jnp.where(high == h, low, zero) for h in range(32)], axis=0)

    def near_work():
        hot = jnp.concatenate([spread(k) for k in range(KA)], axis=1)
        acc[...] = nn(hot, tiles(near_ref, 0, KA))

    def far_work(k, v):
        acc[...] += nn(spread(k), v)

    far_chunks(info_ref, far_hbm, buf, sems, near_work, far_work)
    for i in range(2):
        out_ref[:, 16 * i : 16 * i + 16, :] = (
            acc[:, C * i : C * i + C].reshape(R, 16, C).astype(BF16)
        )


def finish_kernel(in_ref, grad_ref, owned_ref, loss_ref):
    total = in_ref[0, 0:32, :].astype(F32)
    for r in range(1, R):
        total = total + in_ref[r, 0:32, :].astype(F32)
    grad_ref[...] = total
    extra = in_ref[:, 32 : 32 + XR, :].astype(F32)[:, 0, :]
    src = iota((C, E), 0)
    pick = jnp.where((src < 3 * OWN) & ((src & 7) == (iota((C, E), 1) & 7)), 1.0, 0.0)
    wide = nn(extra.astype(BF16), pick.astype(BF16))
    own = lax.shift_right_logical(iota((R, E), 1), 3) == iota((R, E), 0)
    owned_ref[...] = jnp.sum(jnp.where(own, wide, 0.0), axis=0, keepdims=True)
    lane = iota((R, C), 1)
    keep = (lane >= 3 * OWN) & (lane < 3 * OWN + 3)
    total_loss = jnp.sum(jnp.where(keep, extra, 0.0), keepdims=True)
    loss_ref[...] = total_loss * (1.0 / (E * R))


def local(body, out_shapes, in_specs, out_specs, scratch, limit, *args, flags=None):
    return pl.pallas_call(
        body,
        out_shape=out_shapes,
        in_specs=in_specs,
        out_specs=out_specs,
        scratch_shapes=scratch,
        compiler_params=pltpu.CompilerParams(vmem_limit_bytes=limit << 20, flags=flags),
    )(*args)


def near(x):
    return pltpu.with_memory_space_constraint(x, pltpu.VMEM)


def far(x):
    return pltpu.with_memory_space_constraint(x, pltpu.HBM)


def on_device(tile_values, tile_blocks, tile_counts, labels, owner_rank, weights):
    shape = jax.ShapeDtypeStruct
    dma = pltpu.SemaphoreType.DMA
    spread = local(
        spread_weights, pltpu.VMEM((R, B // (2 * R), 2 * C), BF16), [ANY], VMEM,
        [pltpu.VMEM((B // R, C), F32), dma(())], 4, far(weights),
    )
    table = lax.all_to_all(spread, "rows", 0, 0, tiled=True).reshape(B // 2, 2 * C)
    owner_row = far(owner_rank.reshape(1, E))
    label_row = far(labels.reshape(1, E))
    packed, over, ids, ex, info = local(
        pack_tiles,
        (
            pltpu.VMEM((KA * CH, 2 * C), BF16),
            pltpu.HBM((KF * CH, 2 * C), BF16),
            pltpu.VMEM((NCH, 1, CH), I32),
            pltpu.VMEM((NCH, 1, CH), I32),
            pltpu.VMEM((4, E), I32),
        ),
        [ANY, ANY, ANY, ANY, ANY, ANY],
        (VMEM, ANY, VMEM, VMEM, VMEM),
        [
            pltpu.SMEM((E,), I32),
            pltpu.VMEM((1, E), I32),
            pltpu.VMEM((SLOT, E), I32),
            pltpu.VMEM((1, E), I32),
            pltpu.VMEM((1, E), I32),
            pltpu.VMEM((NG, GR, C), BF16),
            pltpu.VMEM((NG + GCH, GR, C), BF16),
            pltpu.VMEM((KF * CH, 2 * C), BF16),
            dma((5,)),
            dma((LOADS,)),
            dma((KF,)),
        ],
        24,
        far(tile_counts.reshape(E)), far(tile_counts.T), far(tile_blocks.T), owner_row, label_row,
        far(tile_values.reshape(NG, GR, C)),
    )
    partial = local(
        margins_kernel, pltpu.VMEM((F, 1, E), F32), [VMEM, VMEM, VMEM, VMEM, VMEM, ANY], VMEM,
        [
            pltpu.VMEM((KF * CH, 2 * C), BF16),
            pltpu.VMEM((E + WIN, C), F32),
            dma((KF,)),
        ],
        16,
        near(info), near(table), near(ids), near(ex), near(packed), far(over),
    )
    parts = lax.all_to_all(partial, "feat", 0, 0, tiled=True)
    payload = local(
        gradient_kernel, pltpu.VMEM((R, B // R + XR, C), BF16),
        [VMEM, VMEM, VMEM, VMEM, VMEM, ANY], VMEM,
        [
            pltpu.VMEM((KF * CH, 2 * C), BF16),
            pltpu.VMEM((B // 2, 2 * C), F32),
            pltpu.VMEM((E + WIN, C), F32),
            dma((KF,)),
        ],
        16,
        near(info), near(parts), near(ids), near(ex), near(packed),
        far(over),
    )
    arrived = lax.all_to_all(payload, "rows", 0, 0, tiled=True)
    gradient, owned, loss = local(
        finish_kernel,
        (shape((B // R, C), F32), shape((1, E), F32), shape((1, 1), F32)),
        [VMEM], (VMEM, VMEM, VMEM), (), 8, near(arrived),
    )
    return owned.reshape(E), gradient, loss.reshape(())


def solution(mesh):
    in_specs = (
        P("rows", "feat", None),
        P("rows", "feat"),
        P("rows", "feat"),
        P("rows"),
        P("rows"),
        P(("feat", "rows"), None),
    )
    out_specs = (P("rows"), P(("feat", "rows"), None), P())
    return jax.shard_map(
        on_device, mesh=mesh, in_specs=in_specs, out_specs=out_specs, check_vma=False
    )
```
